32 devices in a mesh: plane: 4 (over y, x), tile: 8 (over z, core).
Axes of the slice: x: 2, y: 2, z: 4, core: 2. Of those that a mesh axis runs over, the one named last changes fastest.
Arguments:
- visibility: float32 [2, 65536], P(None, ('plane', 'tile')), may hold values from -6 to 6
- target: int32 [65536, 1], P(('plane', 'tile')), may hold values from 0 to 31; in each aligned block of 2048 rows (0 to 2047, 2048 to 4095, ...) at most 128 rows name the same one
- offset: int32 [65536], P(('plane', 'tile')), may hold values from 0 to 2097151
- taps: float32 [8], replicated, may hold values from 0.1 to 1
- w_plane: float32 [4], P('plane'), may hold values from -300 to 300
Outputs:
- dirty_image: float32 [4096, 4096], P('plane', 'tile')
The draws below stay inside these ranges and needn't reach their ends.
Inputs may be any that keep to these rules, and one draw needn't show every extreme that they name: `target`: among the rows of one device no value occurs more than 128 times, and some value occurs exactly 128 times.
All inputs are finite; a program needn't handle non-finite values.
Results may differ from the reference program's by a relative error of at most 0.0042.
Values sent between devices are 32-bit elements; how exact they have to be, the bound alone decides.
A program may use at most 128 MiB of HBM per device.

```python
import math
import jax
import jax.numpy as jnp
import numpy as np
from jax import lax

G = 4096
KS = 8
VIS_DEV = 2048
PLANES = 4
ROWS = 512
CAP = 128
VIS_ALL = 65536
N_PLANE = 4
N_TILE = 8


def plant(entries, key, smallest, largest):
    spot = [jax.random.randint(jax.random.fold_in(key, axis), (), 0, length) for axis, length in enumerate(entries.shape)]
    main_axis = entries.shape.index(max(entries.shape))
    neighbour = spot[:main_axis] + [(spot[main_axis] + 1) % entries.shape[main_axis]] + spot[main_axis + 1:]
    return entries.at[tuple(spot)].set(smallest).at[tuple(neighbour)].set(largest)


def shard_levels(own_key, shape, pieces, low, largest):
    level = 1.0
    for dim, parts in pieces:
        draws = jax.random.uniform(jax.random.fold_in(jax.random.fold_in(own_key, 6), dim), (parts,), jnp.float32, low / len(pieces), largest / len(pieces))
        level = level * jnp.repeat(jnp.exp(draws), shape[dim] // parts).reshape((-1,) + (1,) * (len(shape) - 1 - dim))
    return level


def deal_out(key, own, number, rows, count, top, reach, lean):
    sequence = jax.random.permutation(key, count)
    packed, common = load_shares(count, rows * top, reach, lean, True), load_shares(count, rows * top, reach, lean, False)
    places = jnp.arange(count)

    def named(sizes, rotation):
        used = int((sizes > 0).sum())
        fixed = max(1, used // 4)
        shifted = fixed + (places - fixed + rotation * (used - fixed)) % max(1, count - fixed)
        return jnp.zeros((count,), jnp.int32).at[sequence[jnp.where(places < fixed, places, shifted)]].set(jnp.asarray(sizes, jnp.int32))

    sizes = jnp.where(number % 4 == 0, named(packed, number // 4), named(common, number - number // 4 - 1))
    mixed = jax.random.permutation(jax.random.fold_in(own, 3), count)
    donor, receiver = mixed[0:count // 2 * 2:2], mixed[1:count // 2 * 2:2]
    slack = jnp.minimum(sizes[donor] - 1, reach - sizes[receiver]) // 2
    slack = jnp.where((donor == sequence[0]) | (receiver == sequence[0]) | (sizes[receiver] == 0), 0, jnp.maximum(slack, 0))
    shifted = jax.random.randint(jax.random.fold_in(own, 4), (count // 2,), 0, 1 << 20) % (slack + 1)
    sizes = sizes.at[donor].add(-shifted).at[receiver].add(shifted)
    members = jnp.searchsorted(jnp.cumsum(sizes), jnp.arange(rows * top), side="right").astype(jnp.int32)
    grid = members.reshape(top, rows).T
    grid = grid[jax.random.permutation(jax.random.fold_in(own, 1), rows)]
    rotation = jax.random.randint(jax.random.fold_in(own, 2), (rows, 1), 0, top)
    return jnp.take_along_axis(grid, (jnp.arange(top)[None, :] + rotation) % top, axis=1)


def load_shares(number_of, total, limit, skew, full):
    weights = [(1 << 20) // math.isqrt(grade ** skew) + 1 for grade in range(1, number_of + 1)]
    largest = limit if full else min(limit, max(-(-total // number_of), total * weights[0] // sum(weights)))
    least = 1 if total - largest >= number_of - 1 else 0
    holding, spare = [largest] + [least] * (number_of - 1), total - largest - least * (number_of - 1)
    while spare > 0:
        free = [i for i in range(1, number_of) if holding[i] < largest] or [i for i in range(1, number_of) if holding[i] < limit]
        pool, budget = sum([weights[i] for i in free]), spare
        for i in free:
            more = min(limit - holding[i], max(1, budget * weights[i] // pool), spare)
            holding[i] = holding[i] + more
            spare = spare - more
    return np.array(holding)


def gaussian(rng, shape, deviation, most, shards=(), kind=jnp.bfloat16):
    result = deviation * jax.random.normal(rng, shape, jnp.float32)
    if shards:
        result = result * shard_levels(rng, shape, shards, -0.22, 0.18)
    return jnp.clip(result, -most, most).astype(kind)


def setup_inputs(seed: int = 0) -> dict:
    keys = jax.random.split(jax.random.key(seed), 6)
    visibility = gaussian(keys[0], (2, VIS_ALL), 1.0, 6.0, ((1, 32),), jnp.float32)
    target_keys = jax.random.split(jax.random.fold_in(keys[1], 1), VIS_ALL // VIS_DEV)
    target_turns = jax.random.permutation(jax.random.fold_in(keys[1], 3), VIS_ALL // VIS_DEV)
    target = jax.vmap(lambda own, number: deal_out(jax.random.fold_in(keys[1], 2), own, number, VIS_DEV, N_PLANE * N_TILE, 1, CAP, 2))(target_keys, target_turns).reshape((VIS_ALL, 1))
    offset = plant(jax.random.randint(keys[2], (VIS_ALL,), 0, ROWS * G), jax.random.fold_in(keys[2], 1), 0, (ROWS * G) - 1).astype(jnp.int32)
    taps = jnp.clip(jnp.exp(jax.random.uniform(keys[3], (KS,), jnp.float32, math.log(0.1), math.log(1.0))), 0.1, 1.0)
    w_plane = jnp.clip(jax.random.uniform(keys[4], (PLANES,), jnp.float32, -300.0, 300.0) * shard_levels(keys[4], (PLANES,), ((0, 4),), -0.4, 0.0), -300.0, 300.0)
    return dict(visibility=visibility, target=target, offset=offset, taps=taps, w_plane=w_plane)


def direction(index, length):
    return ((index + length // 2) % length - length // 2).astype(jnp.float32) * (0.5 / length)

def reference(visibility, target, offset, taps, w_plane):
    destination = target[:, 0]
    plane_of = destination // N_TILE
    tile_of = destination % N_TILE
    grid_row = tile_of * (G // N_TILE) + offset // G
    grid_col = offset % G
    kernel_len = taps.shape[0]
    count = visibility.shape[1]
    weight_re = lax.optimization_barrier((taps[None, :] * visibility[0][:, None]).astype(jnp.bfloat16)).astype(jnp.float32)
    weight_im = lax.optimization_barrier((taps[None, :] * visibility[1][:, None]).astype(jnp.bfloat16)).astype(jnp.float32)
    taps_round = lax.optimization_barrier(taps.astype(jnp.bfloat16)).astype(jnp.float32)
    shifts = jnp.arange(kernel_len, dtype=jnp.int32)
    row_index = (grid_row[:, None] + shifts[None, :]) % G
    col_index = (grid_col[:, None] + shifts[None, :]) % G
    row_full = jnp.broadcast_to(row_index[:, :, None], (count, kernel_len, kernel_len))
    col_full = jnp.broadcast_to(col_index[:, None, :], (count, kernel_len, kernel_len))
    lines = jnp.arange(G, dtype=jnp.int32)
    cosines = direction(lines, G)
    n_minus = jnp.sqrt(1.0 - cosines[:, None] * cosines[:, None] - cosines[None, :] * cosines[None, :]) - 1.0
    image = jnp.zeros((G, G), jnp.float32)
    for plane in range(N_PLANE):
        mask = (plane_of == plane).astype(jnp.float32)
        value_re = (weight_re * mask[:, None])[:, :, None] * taps_round[None, None, :]
        value_im = (weight_im * mask[:, None])[:, :, None] * taps_round[None, None, :]
        grid_re = jnp.zeros((G, G), jnp.float32).at[row_full, col_full].add(value_re)
        grid_im = jnp.zeros((G, G), jnp.float32).at[row_full, col_full].add(value_im)
        transformed = jnp.fft.ifft2(grid_re + 1j * grid_im) * (G * G)
        phase = 2.0 * math.pi * w_plane[plane] * n_minus
        image = image + (jnp.cos(phase) * jnp.real(transformed) - jnp.sin(phase) * jnp.imag(transformed))
    return image * (1.0 / math.sqrt(VIS_ALL))
```

```python
import functools
import math

import jax
import jax.numpy as jnp
import numpy as np
from jax import lax
from jax.experimental import pallas as pl
from jax.experimental.pallas import tpu as pltpu
from jax.sharding import PartitionSpec as P

G = 4096
LANES = 128
WINDOW = 256
DIGITS = G // WINDOW
BLOCK = 64
WIDE = 512
NARROW = 256
MESH = pl.DeviceIdType.MESH


def fitted(function, terms):
    nodes = np.cos((np.arange(400) + 0.5) * np.pi / 400)
    square = 0.125 * (nodes + 1.0)
    table = np.polynomial.chebyshev.Chebyshev.fit(
        square, function(np.sqrt(square)), terms - 1, domain=[0.0, 0.25]
    )
    return [float(v) for v in table.convert(kind=np.polynomial.Polynomial).coef]


COS_COEF = fitted(lambda x: np.cos(2.0 * np.pi * x), 7)
SIN_COEF = fitted(lambda x: np.sin(2.0 * np.pi * x) / x, 6)


def horner(coefficients, x):
    total = coefficients[-1]
    for value in coefficients[-2::-1]:
        total = total * x + value
    return total


def turn(cycles):
    part = cycles - jnp.round(cycles)
    square = part * part
    return horner(COS_COEF, square), part * horner(SIN_COEF, square)


def pieces(value):
    high = value.astype(jnp.bfloat16).astype(jnp.float32)
    rest = value - high
    middle = rest.astype(jnp.bfloat16).astype(jnp.float32)
    return high, middle, rest - middle


def strict_upper(n):
    return jnp.where(
        lax.broadcasted_iota(jnp.int32, (n, n), 0) < lax.broadcasted_iota(jnp.int32, (n, n), 1),
        1.0,
        0.0,
    ).astype(jnp.bfloat16)


NT = (((1,), (1,)), ((), ()))


def pack_kernel(vis_ref, target_ref, offset_ref, out_ref, lhs_ref, rhs_ref):
    buckets, capacity = out_ref.shape[1], out_ref.shape[2]
    blocks = target_ref.shape[0]
    upper = strict_upper(LANES)
    line = lax.broadcasted_iota(jnp.int32, (buckets, LANES), 0)
    slot = lax.broadcasted_iota(jnp.int32, (capacity, LANES), 0).astype(jnp.float32)
    carry = jnp.zeros((buckets, 1), jnp.float32)
    for k in range(blocks):
        part = slice(k * LANES, (k + 1) * LANES)
        hit = line == target_ref[k : k + 1, :]
        hot = jnp.where(hit, 1.0, 0.0)
        before = jnp.dot(hot.astype(jnp.bfloat16), upper, preferred_element_type=jnp.float32)
        rank = jnp.sum(hot * (before + carry), axis=0, keepdims=True)
        carry = carry + jnp.sum(hot, axis=1, keepdims=True)
        rhs_ref[:, part] = jnp.where(slot == rank, 1.0, 0.0).astype(jnp.bfloat16)
        rows = (
            vis_ref[0, k : k + 1, :],
            vis_ref[1, k : k + 1, :],
            offset_ref[k : k + 1, :].astype(jnp.float32) + 1.0,
        )
        for p, row in enumerate(rows):
            for n, value in enumerate(pieces(row)):
                at = (p * 3 + n) * buckets
                lhs_ref[at : at + buckets, part] = jnp.where(hit, value, 0.0).astype(jnp.bfloat16)
    total = lax.dot_general(lhs_ref[...], rhs_ref[...], NT, preferred_element_type=jnp.float32)
    for p in range(3):
        at = p * 3 * buckets
        out_ref[p] = (
            total[at : at + buckets]
            + total[at + buckets : at + 2 * buckets]
            + total[at + 2 * buckets : at + 3 * buckets]
        )


def sort_kernel(windows, in_ref, out_ref, lhs_ref, rhs_ref):
    blocks = in_ref.shape[1]
    slots = blocks * LANES
    encoded = in_ref[2]
    row = jnp.floor((encoded - 1.0) * (1.0 / G))
    upper = strict_upper(LANES)
    lower = jnp.where(
        lax.broadcasted_iota(jnp.int32, (blocks, blocks), 0)
        > lax.broadcasted_iota(jnp.int32, (blocks, blocks), 1),
        1.0,
        0.0,
    ).astype(jnp.bfloat16)
    position = jnp.full(row.shape, -1.0, jnp.float32)
    for w in range(windows):
        member = jnp.where((row >= w * WINDOW) & (row < (w + 1) * WINDOW), 1.0, 0.0)
        flags = member.astype(jnp.bfloat16)
        inside = jnp.dot(flags, upper, preferred_element_type=jnp.float32)
        ahead = jnp.sum(
            jnp.dot(lower, flags, preferred_element_type=jnp.float32), axis=1, keepdims=True
        )
        place = inside + ahead
        if w == 1:
            place = slots - 1 - place
        position = jnp.where(member > 0.0, place, position)
    high = jnp.floor(position * (1.0 / LANES))
    low = position - high * LANES
    line = lax.broadcasted_iota(jnp.int32, (blocks, LANES), 0).astype(jnp.float32)
    slot = lax.broadcasted_iota(jnp.int32, (LANES, LANES), 0).astype(jnp.float32)
    parts = [pieces(in_ref[p]) for p in range(3)]
    for k in range(blocks):
        part = slice(k * LANES, (k + 1) * LANES)
        hit = line == high[k : k + 1, :]
        rhs_ref[:, part] = jnp.where(slot == low[k : k + 1, :], 1.0, 0.0).astype(jnp.bfloat16)
        for p in range(3):
            for n in range(3):
                at = (p * 3 + n) * blocks
                lhs_ref[at : at + blocks, part] = jnp.where(
                    hit, parts[p][n][k : k + 1, :], 0.0
                ).astype(jnp.bfloat16)
    total = lax.dot_general(lhs_ref[...], rhs_ref[...], NT, preferred_element_type=jnp.float32)
    for p in range(3):
        at = p * 3 * blocks
        out_ref[p] = (
            total[at : at + blocks]
            + total[at + blocks : at + 2 * blocks]
            + total[at + 2 * blocks : at + 3 * blocks]
        )


def spread(re, im, leads_cos, leads_sin):
    half = len(leads_cos)
    low, high = [], []
    for cos_l, sin_l in zip(leads_cos, leads_sin):
        a, b = re * cos_l, im * sin_l
        c, d = im * cos_l, re * sin_l
        high.append((a - b, c + d))
        low.append((a + b, c - d))
    assert len(low) == half
    return low[::-1] + high


def grid_kernel(windows, columns, count_ref, first_ref, vis_ref, out_ref, table_ref, hot_ref):
    tile, window = pl.program_id(0), pl.program_id(1)
    blocks = vis_ref.shape[2]
    tops = columns // BLOCK
    number = count_ref[tile * windows + window]
    lowest = (window * WINDOW).astype(jnp.float32)
    base = first_ref[0] + (tops - 1) * (BLOCK // 2) + 28
    eight = lax.broadcasted_iota(jnp.int32, (8, LANES), 0)
    start_at = (eight + base).astype(jnp.float32)
    lead_at = jnp.where(eight < 4, 4 + 8 * eight, 32 + 64 * (eight - 4)).astype(jnp.float32)
    lane = lax.broadcasted_iota(jnp.int32, (LANES, LANES), 1).astype(jnp.float32)

    def build(group, row):
        part = slice(group * LANES, (group + 1) * LANES)
        vis_re = vis_ref[0, 0, pl.ds(row, 1), :]
        vis_im = vis_ref[0, 1, pl.ds(row, 1), :]
        encoded = vis_ref[0, 2, pl.ds(row, 1), :] - 1.0
        line = jnp.floor(encoded * (1.0 / G))
        unit = (encoded - line * G) * (1.0 / G)
        near = jnp.broadcast_to(line - lowest, (LANES, LANES)).T
        hot_ref[part, :LANES] = jnp.where(near == lane, 1.0, 0.0).astype(jnp.bfloat16)
        hot_ref[part, LANES:] = jnp.where(near == lane + LANES, 1.0, 0.0).astype(jnp.bfloat16)
        start_cos, start_sin = turn(start_at * unit)
        lead_cos, lead_sin = turn(lead_at * unit)
        first_re = vis_re * start_cos - vis_im * start_sin
        first_im = vis_re * start_sin + vis_im * start_cos
        small = spread(
            first_re,
            first_im,
            [lead_cos[i : i + 1] for i in range(4)],
            [lead_sin[i : i + 1] for i in range(4)],
        )
        block_re = jnp.concatenate([v[0] for v in small], axis=0)
        block_im = jnp.concatenate([v[1] for v in small], axis=0)
        large = spread(
            block_re,
            block_im,
            [lead_cos[4 + i : 5 + i] for i in range(tops // 2)],
            [lead_sin[4 + i : 5 + i] for i in range(tops // 2)],
        )
        for top, (re, im) in enumerate(large):
            at = top * BLOCK
            table_ref[at : at + BLOCK, part] = re.astype(jnp.bfloat16)
            table_ref[columns + at : columns + at + BLOCK, part] = im.astype(jnp.bfloat16)

    def chunk(row, width):
        for group in range(width // LANES):
            build(group, row + group)
        return jnp.dot(
            table_ref[:, :width], hot_ref[:width, :], preferred_element_type=jnp.float32
        )

    def place(index, width):
        forward = index * (WIDE // LANES)
        return jnp.where(window == 0, forward, blocks - forward - width // LANES)

    out_ref[0] = chunk(place(0, WIDE), WIDE)
    rest = jnp.maximum(number - WIDE, 0)
    full = rest // WIDE
    tail = rest - full * WIDE
    full = full + jnp.where(tail > NARROW, 1, 0)

    @pl.loop(0, full)
    def _(index):
        out_ref[0] += chunk(place(index + 1, WIDE), WIDE)

    @pl.when((tail > 0) & (tail <= NARROW))
    def _():
        out_ref[0] += chunk(place(full + 1, NARROW), NARROW)


def quarter(value, turns):
    re, im = value
    return ((re, im), (-im, re), (-re, -im), (im, -re))[turns % 4]


def plus(left, right):
    return left[0] + right[0], left[1] + right[1]


def minus(left, right):
    return left[0] - right[0], left[1] - right[1]


def image_kernel(held, own, w_ref, weight_ref, twist_ref, line_ref, side_ref, *refs):
    grids, out_ref = refs[:held], refs[held]
    mixed_ref, send_ref, own_ref, got_ref, send_sem, got_sem = refs[held + 1 :]
    step = pl.program_id(0)
    steps = pl.num_programs(0)
    mine = lax.axis_index("plane")
    core = lax.rem(lax.axis_index("tile"), 2)
    near = mine + 1 - 2 * lax.rem(mine, 2)
    far = mine + 2 - 4 * lax.rem(mine // 2, 2)
    partner = near * (1 - core) + far * core
    barrier = pltpu.get_barrier_semaphore()

    @pl.when(step == 0)
    def _():
        pl.semaphore_signal(
            barrier, inc=1, device_id={"plane": partner}, device_id_type=MESH
        )
        pl.semaphore_wait(barrier, 1)

    for k in range(held):
        grid_ref = grids[k]

        @pl.loop(0, LANES // 16)
        def _(index):
            at = pl.multiple_of(index * 16, 16)
            part = pl.ds(at, 16)
            for half in range(WINDOW // LANES):
                lanes = slice(half * LANES, (half + 1) * LANES)
                for b0 in range(4):
                    heads = []
                    for w0 in range(4):
                        total = None
                        for w1 in range(4):
                            w = 4 * w1 + w0
                            value = quarter(
                                (grid_ref[w, 0, part, lanes], grid_ref[w, 1, part, lanes]), w1 * b0
                            )
                            total = value if total is None else plus(total, value)
                        if w0 * b0:
                            angle = 2.0 * math.pi * w0 * b0 / DIGITS
                            c, s = math.cos(angle), math.sin(angle)
                            re, im = total
                            total = (re * c - im * s, re * s + im * c)
                        heads.append(total)
                    even, odd = plus(heads[0], heads[2]), minus(heads[0], heads[2])
                    even2, odd2 = plus(heads[1], heads[3]), minus(heads[1], heads[3])
                    odd2 = quarter(odd2, 1)
                    results = (plus(even, even2), plus(odd, odd2), minus(even, even2), minus(odd, odd2))
                    for b1, (re, im) in enumerate(results):
                        b = b0 + 4 * b1
                        if b:
                            c = twist_ref[0, b : b + 1, lanes]
                            s = twist_ref[1, b : b + 1, lanes]
                            re, im = re * c - im * s, re * s + im * c
                        mixed_ref[b, pl.ds(k * LANES + at, 16), lanes] = re.astype(jnp.bfloat16)
                        mixed_ref[
                            b,
                            pl.ds(k * LANES + at, 16),
                            WINDOW + half * LANES : WINDOW + (half + 1) * LANES,
                        ] = im.astype(jnp.bfloat16)

    lanes = pl.ds(pl.multiple_of(step * LANES, LANES), LANES)
    flat_m = side_ref[:, 0:1]
    angle_m = side_ref[:, 1:2]
    size_m = side_ref[:, 2:3]
    width = line_ref.shape[2]

    @pl.loop(0, DIGITS)
    def _(b):
        full = jnp.dot(mixed_ref[b], weight_ref[...], preferred_element_type=jnp.float32)
        flat = line_ref[0, pl.ds(b, 1), :]
        angle = line_ref[1, pl.ds(b, 1), :] + angle_m
        drop = jnp.sqrt(flat - flat_m) - 1.0
        picture = None
        for k in range(held):
            rows = slice(k * LANES, (k + 1) * LANES)
            cos_s, sin_s = turn(w_ref[k] * drop + angle)
            value = cos_s * full[rows, :width] - sin_s * full[rows, width:]
            picture = value if picture is None else picture + value
        picture = (picture * (line_ref[2, pl.ds(b, 1), :] * size_m)).T
        send_ref[step, b] = picture[:own]
        own_ref[b, :, lanes] = picture[own : 2 * own]

    def copy(index):
        return pltpu.make_async_remote_copy(
            src_ref=send_ref.at[index],
            dst_ref=got_ref.at[index],
            send_sem=send_sem.at[index],
            recv_sem=got_sem.at[index],
            device_id={"plane": partner},
            device_id_type=MESH,
        )

    copy(step).start()

    @pl.when(step == steps - 1)
    def _():
        for index in range(send_ref.shape[0]):
            copy(index).wait()
            block = slice(index * LANES, (index + 1) * LANES)

            for b in range(DIGITS):
                out_ref[:, b, block] = own_ref[b, :, block] + got_ref[index, b]


def direction(index, length):
    return ((index + length // 2) % length - length // 2).astype(jnp.float32) * (0.5 / length)


def response(taps, index):
    shifts = jnp.arange(taps.shape[0], dtype=jnp.int32).reshape((-1,) + (1,) * index.ndim)
    angles = (shifts * index[None] % G).astype(jnp.float32) * (2.0 * math.pi / G)
    weights = taps.reshape(shifts.shape)
    real = jnp.sum(jnp.cos(angles) * weights, axis=0)
    imag = jnp.sum(jnp.sin(angles) * weights, axis=0)
    return jnp.arctan2(imag, real) * (0.5 / math.pi), jnp.sqrt(real * real + imag * imag)


def local(visibility, target, offset, taps, w_plane):
    tiles = lax.axis_size("tile")
    planes = lax.axis_size("plane")
    devices = tiles * planes
    vis_dev = visibility.shape[1]
    capacity = 2 * vis_dev // devices
    slots = devices * capacity
    blocks = slots // LANES
    band = G // tiles
    columns = G // tiles
    windows = band // WINDOW
    own = G // planes // DIGITS
    width = max(LANES, 2 * own)
    held = planes // 2
    assert windows in (1, 2)
    vmem = pl.BlockSpec(memory_space=pltpu.VMEM)
    smem = pl.BlockSpec(memory_space=pltpu.SMEM)

    outgoing = pl.pallas_call(
        pack_kernel,
        out_shape=jax.ShapeDtypeStruct((3, devices, capacity), jnp.float32),
        in_specs=[vmem] * 3,
        out_specs=vmem,
        scratch_shapes=[
            pltpu.VMEM((9 * devices, vis_dev), jnp.bfloat16),
            pltpu.VMEM((capacity, vis_dev), jnp.bfloat16),
        ],
    )(
        visibility.reshape(2, -1, LANES),
        target.reshape(-1, LANES),
        offset.reshape(-1, LANES),
    )
    received = lax.all_to_all(
        outgoing, ("plane", "tile"), split_axis=1, concat_axis=1, tiled=True
    ).reshape(3, blocks, LANES)
    ordered = pl.pallas_call(
        functools.partial(sort_kernel, windows),
        out_shape=jax.ShapeDtypeStruct((3, blocks, LANES), jnp.float32),
        in_specs=[vmem],
        out_specs=vmem,
        scratch_shapes=[
            pltpu.VMEM((9 * blocks, slots), jnp.bfloat16),
            pltpu.VMEM((LANES, slots), jnp.bfloat16),
        ],
    )(received)
    gathered = lax.all_gather(ordered, "tile", axis=0)

    mine = lax.axis_index("plane")
    tile = lax.axis_index("tile")
    first = (tile * columns).astype(jnp.int32)
    core = tile % 2
    partner = jnp.where(core == 0, mine ^ 1, mine ^ 2)

    numbers = np.arange(planes)
    jumps = [[d for d in numbers if not d & bit] for bit in (1, 2)]
    lists, levels = [gathered], [w_plane]
    for k in range(1, held):
        moves = []
        for q in range(planes):
            for t in range(tiles):
                moves.append((q * tiles + t, int(q ^ jumps[t % 2][k]) * tiles + t))
        lists.append(lax.ppermute(gathered, ("plane", "tile"), moves))
        levels.append(lax.ppermute(w_plane, ("plane", "tile"), moves))

    def transform(slots_of):
        line = jnp.floor((slots_of[:, 2] - 1.0) * (1.0 / G))
        counts = jnp.stack(
            [
                jnp.sum(
                    ((line >= w * WINDOW) & (line < (w + 1) * WINDOW)).astype(jnp.int32),
                    axis=(1, 2),
                )
                for w in range(windows)
            ],
            axis=1,
        ).reshape(-1)
        return pl.pallas_call(
            functools.partial(grid_kernel, windows, columns),
            grid=(tiles, windows),
            out_shape=jax.ShapeDtypeStruct((DIGITS, 2 * columns, WINDOW), jnp.float32),
            in_specs=[
                smem,
                smem,
                pl.BlockSpec((1, 3, blocks, LANES), lambda t, w: (t, 0, 0, 0)),
            ],
            out_specs=pl.BlockSpec(
                (1, 2 * columns, WINDOW), lambda t, w: (t * windows + w, 0, 0)
            ),
            scratch_shapes=[
                pltpu.VMEM((2 * columns, WIDE), jnp.bfloat16),
                pltpu.VMEM((WIDE, WINDOW), jnp.bfloat16),
            ],
            cost_estimate=pl.CostEstimate(
                flops=2 * slots * tiles * columns * WINDOW, bytes_accessed=1 << 24, transcendentals=0
            ),
        )(counts, first[None], slots_of).reshape(DIGITS, 2, columns, WINDOW)

    grids = [transform(v) for v in lists]

    parts = np.arange(width)
    starts = jnp.stack([partner, mine]) * own
    place = jnp.where(
        parts < own, starts[0] + parts, starts[1] + jnp.asarray(parts) - own
    ).astype(jnp.int32)
    place = place % WINDOW
    inner = jnp.arange(WINDOW, dtype=jnp.int32)
    angles = (inner[:, None] * place[None, :] % WINDOW).astype(jnp.float32) * (1.0 / WINDOW)
    cos_d, sin_d = turn(angles)
    weight = jnp.block([[cos_d, sin_d], [-sin_d, cos_d]]).astype(jnp.bfloat16)
    digits = np.arange(DIGITS)
    angles = 2.0 * np.pi * (digits[:, None] * np.arange(WINDOW)[None, :]) / G
    twist = jnp.asarray(np.stack([np.cos(angles), np.sin(angles)]).astype(np.float32))

    line_pos = DIGITS * place[None, :] + jnp.arange(DIGITS, dtype=jnp.int32)[:, None]
    line_angle, line_size = response(taps, line_pos)
    cos_row = direction(line_pos, G)
    line = jnp.stack(
        [1.0 - cos_row * cos_row, line_angle, line_size * (1.0 / math.sqrt(vis_dev * devices))]
    )
    column_pos = first + jnp.arange(columns, dtype=jnp.int32)
    side_angle, side_size = response(taps.astype(jnp.bfloat16).astype(jnp.float32), column_pos)
    cos_col = direction(column_pos, G)
    side = jnp.stack([cos_col * cos_col, side_angle, side_size], axis=1)

    steps = columns // LANES
    image = pl.pallas_call(
        functools.partial(image_kernel, held, own),
        grid=(steps,),
        out_shape=jax.ShapeDtypeStruct((own, DIGITS, columns), jnp.float32),
        in_specs=[
            smem,
            vmem,
            vmem,
            vmem,
            pl.BlockSpec((LANES, 3), lambda j: (j, 0)),
        ]
        + [pl.BlockSpec((DIGITS, 2, LANES, WINDOW), lambda j: (0, 0, j, 0))] * held,
        out_specs=pl.BlockSpec((own, DIGITS, columns), lambda j: (0, 0, 0)),
        scratch_shapes=[
            pltpu.VMEM((DIGITS, held * LANES, 2 * WINDOW), jnp.bfloat16),
            pltpu.VMEM((steps, DIGITS, own, LANES), jnp.float32),
            pltpu.VMEM((DIGITS, own, columns), jnp.float32),
            pltpu.VMEM((steps, DIGITS, own, LANES), jnp.float32),
            pltpu.SemaphoreType.DMA((steps,)),
            pltpu.SemaphoreType.DMA((steps,)),
        ],
        compiler_params=pltpu.CompilerParams(
            collective_id=0,
            has_side_effects=True,
            vmem_limit_bytes=60 * 1024 * 1024,
            dimension_semantics=("arbitrary",),
        ),
    )(jnp.concatenate(levels), weight, twist, line, side, *grids)
    return image.reshape(own * DIGITS, columns)


def solution(mesh):
    return jax.shard_map(
        local,
        mesh=mesh,
        in_specs=(
            P(None, ("plane", "tile")),
            P(("plane", "tile"), None),
            P(("plane", "tile")),
            P(),
            P("plane"),
        ),
        out_specs=P("plane", "tile"),
        check_vma=False,
    )
```

```python
import functools
import math

import jax
import jax.numpy as jnp
import numpy as np
from jax import lax
from jax.experimental import pallas as pl
from jax.experimental.pallas import tpu as pltpu
from jax.sharding import PartitionSpec as P

G = 4096
LANES = 128
WINDOW = 256
DIGITS = G // WINDOW
BLOCK = 64
PIECE = 4
WIDE = 1024
HALF = 512
NARROW = 256
MESH = pl.DeviceIdType.MESH


def fitted(function, terms):
    nodes = np.cos((np.arange(400) + 0.5) * np.pi / 400)
    square = 0.125 * (nodes + 1.0)
    table = np.polynomial.chebyshev.Chebyshev.fit(
        square, function(np.sqrt(square)), terms - 1, domain=[0.0, 0.25]
    )
    return [float(v) for v in table.convert(kind=np.polynomial.Polynomial).coef]


COS_COEF = fitted(lambda x: np.cos(2.0 * np.pi * x), 7)
SIN_COEF = fitted(lambda x: np.sin(2.0 * np.pi * x) / x, 6)


SHORT_COS = fitted(lambda x: np.cos(2.0 * np.pi * x), 6)
SHORT_SIN = fitted(lambda x: np.sin(2.0 * np.pi * x) / x, 5)


def horner(coefficients, x):
    total = coefficients[-1]
    for value in coefficients[-2::-1]:
        total = total * x + value
    return total


def turn(cycles, cos_terms=COS_COEF, sin_terms=SIN_COEF):
    part = cycles - jnp.round(cycles)
    square = part * part
    return horner(cos_terms, square), part * horner(sin_terms, square)


def pieces(value):
    high = value.astype(jnp.bfloat16).astype(jnp.float32)
    rest = value - high
    middle = rest.astype(jnp.bfloat16).astype(jnp.float32)
    return high, middle, rest - middle


def strict_upper(n):
    return jnp.where(
        lax.broadcasted_iota(jnp.int32, (n, n), 0) < lax.broadcasted_iota(jnp.int32, (n, n), 1),
        1.0,
        0.0,
    ).astype(jnp.bfloat16)


NT = (((1,), (1,)), ((), ()))


def flip(value, bits):
    bit = 1
    while bit <= bits:
        if bits & bit:
            value = value + bit - 2 * bit * lax.rem(value // bit, 2)
        bit *= 2
    return value


def front_kernel(
    windows, tiles, jumps, vis_ref, target_ref, offset_ref, w_ref, out_ref, level_ref,
    lhs_ref, rhs_ref, left_ref, right_ref, send_ref, got_ref, ring_ref,
    send_sem, got_sem, pass_sem, ring_sem,
):
    devices = send_ref.shape[0]
    plane, tile = lax.axis_index("plane"), lax.axis_index("tile")
    mine = plane * tiles + tile
    barrier = pltpu.get_barrier_semaphore()

    def seat(device):
        return {"plane": device // tiles, "tile": lax.rem(device, tiles)}

    @pl.loop(1, devices)
    def _(i):
        pl.semaphore_signal(
            barrier, inc=1, device_id=seat(lax.rem(mine + i, devices)), device_id_type=MESH
        )

    blocks = target_ref.shape[0]
    upper = strict_upper(LANES)
    line = lax.broadcasted_iota(jnp.int32, (devices, LANES), 0)
    slot = lax.broadcasted_iota(jnp.int32, (LANES, LANES), 0).astype(jnp.float32)
    carry = jnp.zeros((devices, 1), jnp.float32)
    for k in range(blocks):
        part = slice(k * LANES, (k + 1) * LANES)
        hit = line == target_ref[k : k + 1, :]
        hot = jnp.where(hit, 1.0, 0.0)
        before = jnp.dot(hot.astype(jnp.bfloat16), upper, preferred_element_type=jnp.float32)
        rank = jnp.sum(hot * (before + carry), axis=0, keepdims=True)
        carry = carry + jnp.sum(hot, axis=1, keepdims=True)
        rhs_ref[:, part] = jnp.where(slot == rank, 1.0, 0.0).astype(jnp.bfloat16)
        rows = (
            vis_ref[0, k : k + 1, :],
            vis_ref[1, k : k + 1, :],
            offset_ref[k : k + 1, :].astype(jnp.float32) + 1.0,
        )
        for p, row in enumerate(rows):
            for n, value in enumerate(pieces(row)):
                at = (p * 3 + n) * devices
                lhs_ref[at : at + devices, part] = jnp.where(hit, value, 0.0).astype(jnp.bfloat16)
    total = lax.dot_general(lhs_ref[...], rhs_ref[...], NT, preferred_element_type=jnp.float32)
    for p in range(3):
        at = p * 3 * devices
        send_ref[:, p, :] = (
            total[at : at + devices]
            + total[at + devices : at + 2 * devices]
            + total[at + 2 * devices : at + 3 * devices]
        )
    send_ref[:, 3, :] = jnp.full((devices, LANES), w_ref[0], jnp.float32)
    got_ref[mine] = send_ref[mine]
    pl.semaphore_wait(barrier, devices - 1)

    def post(source, target):
        return pltpu.make_async_remote_copy(
            src_ref=send_ref.at[target],
            dst_ref=got_ref.at[source],
            send_sem=send_sem.at[target],
            recv_sem=got_sem.at[source],
            device_id=seat(target),
            device_id_type=MESH,
        )

    @pl.loop(1, devices)
    def _(i):
        post(mine, lax.rem(mine + i, devices)).start()

    @pl.loop(1, devices)
    def _(i):
        post(lax.rem(mine + devices - i, devices), mine).wait_recv()

    for k in range(level_ref.shape[0]):
        near, far = flip(plane, jumps[0][k]), flip(plane, jumps[1][k])
        core = lax.rem(tile, 2)
        origin = (near * (1 - core) + far * core) * tiles + tile
        level_ref[k : k + 1, :] = got_ref[origin, 3:4, :]

    rows = out_ref.shape[2]
    encoded = got_ref[:, 2, :]
    row = jnp.floor((encoded - 1.0) * (1.0 / G))
    lower = jnp.where(
        lax.broadcasted_iota(jnp.int32, (devices, devices), 0)
        > lax.broadcasted_iota(jnp.int32, (devices, devices), 1),
        1.0,
        0.0,
    ).astype(jnp.bfloat16)
    position = jnp.full(row.shape, -1.0, jnp.float32)
    for w in range(windows):
        member = jnp.where((row >= w * WINDOW) & (row < (w + 1) * WINDOW), 1.0, 0.0)
        flags = member.astype(jnp.bfloat16)
        inside = jnp.dot(flags, upper, preferred_element_type=jnp.float32)
        ahead = jnp.sum(
            jnp.dot(lower, flags, preferred_element_type=jnp.float32), axis=1, keepdims=True
        )
        place = inside + ahead
        if w == 1:
            place = rows * LANES - 1 - place
        position = jnp.where(member > 0.0, place, position)
    high = jnp.floor(position * (1.0 / LANES))
    low = position - high * LANES
    line = lax.broadcasted_iota(jnp.int32, (rows, LANES), 0).astype(jnp.float32)
    parts = [pieces(got_ref[:, 0, :]), pieces(got_ref[:, 1, :]), pieces(encoded)]
    for k in range(devices):
        part = slice(k * LANES, (k + 1) * LANES)
        hit = line == high[k : k + 1, :]
        right_ref[:, part] = jnp.where(slot == low[k : k + 1, :], 1.0, 0.0).astype(jnp.bfloat16)
        for p in range(3):
            for n in range(3):
                at = (p * 3 + n) * rows
                left_ref[at : at + rows, part] = jnp.where(
                    hit, parts[p][n][k : k + 1, :], 0.0
                ).astype(jnp.bfloat16)
    total = lax.dot_general(left_ref[...], right_ref[...], NT, preferred_element_type=jnp.float32)
    for p in range(3):
        at = p * 3 * rows
        ring_ref[tile, p] = (
            total[at : at + rows]
            + total[at + rows : at + 2 * rows]
            + total[at + 2 * rows : at + 3 * rows]
        )

    sister = tile + 1 - 2 * lax.rem(tile, 2)

    def hand(block, target, index):
        return pltpu.make_async_remote_copy(
            src_ref=ring_ref.at[block],
            dst_ref=ring_ref.at[block],
            send_sem=pass_sem.at[index],
            recv_sem=ring_sem.at[block],
            device_id={"tile": target},
            device_id_type=MESH,
        )

    steps = tiles // 2
    hand(tile, sister, 0).start()
    for i in range(1, steps):
        hand(tile, lax.rem(tile + 2 * i, tiles), i).start()
    for i in range(1, steps):
        block = lax.rem(tile + tiles - 2 * i, tiles)
        hand(block, sister, 0).wait_recv()
        hand(block, sister, steps + i).start()
    hand(sister, sister, 0).wait_recv()
    for i in range(1, steps):
        hand(lax.rem(sister + tiles - 2 * i, tiles), sister, 0).wait_recv()
    out_ref[...] = ring_ref[...]
    hand(tile, sister, 0).wait_send()
    for i in range(1, steps):
        hand(tile, lax.rem(tile + 2 * i, tiles), i).wait_send()
        hand(tile, sister, steps + i).wait_send()

    @pl.loop(1, devices)
    def _(i):
        post(mine, lax.rem(mine + i, devices)).wait_send()


def spread(re, im, leads_cos, leads_sin):
    half = len(leads_cos)
    low, high = [], []
    for cos_l, sin_l in zip(leads_cos, leads_sin):
        a, b = re * cos_l, im * sin_l
        c, d = im * cos_l, re * sin_l
        high.append((a - b, c + d))
        low.append((a + b, c - d))
    assert len(low) == half
    return low[::-1] + high


def grid_kernel(windows, columns, count_ref, first_ref, vis_ref, out_ref, table_ref, hot_ref, near_ref, lead_ref):
    tile, window = pl.program_id(0), pl.program_id(1)
    blocks = vis_ref.shape[2]
    tops = columns // BLOCK
    number = count_ref[tile, window]
    lowest = (window * WINDOW).astype(jnp.float32)
    base = first_ref[0] + (tops - 1) * (BLOCK // 2) + 28
    eight = lax.broadcasted_iota(jnp.int32, (8, LANES), 0)
    start_at = (eight + base).astype(jnp.float32)
    lead_at = jnp.where(eight < 4, 4 + 8 * eight, 32 + 64 * (eight - 4)).astype(jnp.float32)
    lane = lax.broadcasted_iota(jnp.int32, (WINDOW, LANES), 0).astype(jnp.float32)

    def build(group, row):
        part = slice(group * LANES, (group + 1) * LANES)
        vis_re = vis_ref[0, 0, pl.ds(row, 1), :]
        vis_im = vis_ref[0, 1, pl.ds(row, 1), :]
        encoded = vis_ref[0, 2, pl.ds(row, 1), :] - 1.0
        line = jnp.floor(encoded * (1.0 / G))
        unit = (encoded - line * G) * (1.0 / G)
        hot_ref[group] = jnp.where(lane == line - lowest, 1.0, 0.0).astype(jnp.bfloat16)
        start_cos, start_sin = turn(start_at * unit)
        lead_cos, lead_sin = turn(lead_at * unit)
        first_re = vis_re * start_cos - vis_im * start_sin
        first_im = vis_re * start_sin + vis_im * start_cos
        small = spread(
            first_re,
            first_im,
            [lead_cos[i : i + 1] for i in range(4)],
            [lead_sin[i : i + 1] for i in range(4)],
        )
        for i, (re, im) in enumerate(small):
            near_ref[0, 8 * i : 8 * i + 8, part] = re
            near_ref[1, 8 * i : 8 * i + 8, part] = im
        lead_ref[0, :, part] = lead_cos
        lead_ref[1, :, part] = lead_sin

    def widen(group):
        part = slice(group * LANES, (group + 1) * LANES)
        for i in range(tops // 2):
            cos_l = lead_ref[0, 4 + i : 5 + i, part]
            sin_l = lead_ref[1, 4 + i : 5 + i, part]
            for lines in range(0, BLOCK, 16):
                re = near_ref[0, lines : lines + 16, part]
                im = near_ref[1, lines : lines + 16, part]
                a, b = re * cos_l, im * sin_l
                c, d = im * cos_l, re * sin_l
                at = (i * BLOCK + lines) * 4
                for n, value in enumerate((a - b, a + b, c + d, c - d)):
                    table_ref[group, at + 16 * n : at + 16 * n + 16, :] = value.astype(
                        jnp.bfloat16
                    )

    def deliver(product, add):
        for i in range(tops // 2):
            for lines in range(0, BLOCK, 16):
                high = (tops // 2 + i) * BLOCK + lines
                low = (tops // 2 - 1 - i) * BLOCK + lines
                at = (i * BLOCK + lines) * 4
                for n, row in enumerate((high, low, columns + high, columns + low)):
                    value = product[at + 16 * n : at + 16 * n + 16]
                    if add:
                        value = value + out_ref[0, row : row + 16]
                    out_ref[0, row : row + 16] = value

    def chunk(row, width, add):
        for group in range(width // LANES):
            build(group, row + group)
        for group in range(width // LANES):
            widen(group)
        groups = range(width // LANES)
        left = jnp.concatenate([table_ref[group] for group in groups], axis=1)
        right = jnp.concatenate([hot_ref[group] for group in groups], axis=1)
        deliver(lax.dot_general(left, right, NT, preferred_element_type=jnp.float32), add)

    def place(done, width):
        return jnp.where(window == 0, done, blocks - done - width // LANES)

    @pl.when(number <= NARROW)
    def _():
        chunk(place(0, NARROW), NARROW, False)

    @pl.when((number > NARROW) & (number <= HALF))
    def _():
        chunk(place(0, HALF), HALF, False)

    @pl.when((number > HALF) & (number <= HALF + NARROW))
    def _():
        chunk(place(0, HALF + NARROW), HALF + NARROW, False)

    @pl.when(number > HALF + NARROW)
    def _():
        chunk(place(0, WIDE), WIDE, False)

    rest = jnp.maximum(number - WIDE, 0)
    full = rest // WIDE
    tail = rest - full * WIDE
    full = full + jnp.where(tail > HALF, 1, 0)

    @pl.loop(0, full)
    def _(index):
        chunk(place((index + 1) * (WIDE // LANES), WIDE), WIDE, True)

    done = (full + 1) * (WIDE // LANES)

    @pl.when((tail > NARROW) & (tail <= HALF))
    def _():
        chunk(place(done, HALF), HALF, True)

    @pl.when((tail > 0) & (tail <= NARROW))
    def _():
        chunk(place(done, NARROW), NARROW, True)


def place(lane, first, second, count):
    return lax.rem(jnp.where(lane < count, first * count + lane, second * count + lane - count), WINDOW)


def squared(index):
    cosine = jnp.where(index >= G // 2, index - G, index).astype(jnp.float32) * (0.5 / G)
    return cosine * cosine


def response(taps, index):
    real = imag = None
    for j, tap in enumerate(taps):
        cos_j, sin_j = turn((index * j).astype(jnp.float32) * (1.0 / G))
        real = tap * cos_j if real is None else real + tap * cos_j
        imag = tap * sin_j if imag is None else imag + tap * sin_j
    return jnp.arctan2(imag, real) * (0.5 / math.pi), jnp.sqrt(real * real + imag * imag)


def quarter(value, turns):
    re, im = value
    return ((re, im), (-im, re), (-re, -im), (im, -re))[turns % 4]


def plus(left, right):
    return left[0] + right[0], left[1] + right[1]


def minus(left, right):
    return left[0] - right[0], left[1] - right[1]


def image_kernel(held, own, columns, scale, taps_ref, w_ref, twist_ref, *refs):
    grids, own_ref, got_ref = refs[:held], refs[held], refs[held + 1]
    mixed_ref, even_ref, odd_ref, send_ref, weight_ref, line_ref, side_ref = refs[held + 2 : -2]
    send_sem, got_sem = refs[-2:]
    width = line_ref.shape[2]
    step = pl.program_id(0)
    steps = pl.num_programs(0)
    mine = lax.axis_index("plane")
    core = lax.rem(lax.axis_index("tile"), 2)
    near = mine + 1 - 2 * lax.rem(mine, 2)
    far = mine + 2 - 4 * lax.rem(mine // 2, 2)
    partner = near * (1 - core) + far * core
    barrier = pltpu.get_barrier_semaphore()

    @pl.when(step == 0)
    def _():
        pl.semaphore_signal(
            barrier, inc=1, device_id={"plane": partner}, device_id_type=MESH
        )
        lane = lax.broadcasted_iota(jnp.int32, (DIGITS, width), 1)
        digit = lax.broadcasted_iota(jnp.int32, (DIGITS, width), 0)
        index = place(lane, partner, mine, own) * DIGITS + digit
        taps = [taps_ref[j] for j in range(taps_ref.shape[0])]
        angle, size = response(taps, index)
        line_ref[0] = 1.0 - squared(index)
        line_ref[1] = angle
        line_ref[2] = size * scale

        @pl.loop(0, WINDOW // 16)
        def _(i):
            at = pl.multiple_of(i * 16, 16)
            lane = lax.broadcasted_iota(jnp.int32, (16, width), 1)
            inner = lax.broadcasted_iota(jnp.int32, (16, width), 0) + at
            product = inner * place(lane, partner, mine, own)
            cos_d, sin_d = turn(product.astype(jnp.float32) * (1.0 / WINDOW))
            weight_ref[pl.ds(at, 16), :width] = cos_d.astype(jnp.bfloat16)
            weight_ref[pl.ds(at, 16), width:] = sin_d.astype(jnp.bfloat16)
            weight_ref[pl.ds(WINDOW + at, 16), :width] = (-sin_d).astype(jnp.bfloat16)
            weight_ref[pl.ds(WINDOW + at, 16), width:] = cos_d.astype(jnp.bfloat16)

        pl.semaphore_wait(barrier, 1)

    index = lax.axis_index("tile") * columns + step * LANES
    index = index + lax.broadcasted_iota(jnp.int32, (8, LANES), 1)
    taps = [
        jnp.full((8, LANES), taps_ref[j], jnp.float32).astype(jnp.bfloat16).astype(jnp.float32)
        for j in range(taps_ref.shape[0])
    ]
    angle, size = response(taps, index)
    for n, value in enumerate((squared(index), angle, size)):
        side_ref[n] = jnp.broadcast_to(value[0:1], (LANES, LANES)).T

    for k in range(held):
        grid_ref = grids[k]

        @pl.loop(0, LANES // 16)
        def _(index):
            at = pl.multiple_of(index * 16, 16)
            part = pl.ds(at, 16)
            for half in range(WINDOW // LANES):
                lanes = slice(half * LANES, (half + 1) * LANES)
                for b0 in range(4):
                    heads = []
                    for w0 in range(4):
                        total = None
                        for w1 in range(4):
                            w = 4 * w1 + w0
                            value = quarter(
                                (grid_ref[w, 0, part, lanes], grid_ref[w, 1, part, lanes]), w1 * b0
                            )
                            total = value if total is None else plus(total, value)
                        if w0 * b0:
                            angle = 2.0 * math.pi * w0 * b0 / DIGITS
                            c, s = math.cos(angle), math.sin(angle)
                            re, im = total
                            total = (re * c - im * s, re * s + im * c)
                        heads.append(total)
                    even, odd = plus(heads[0], heads[2]), minus(heads[0], heads[2])
                    even2, odd2 = plus(heads[1], heads[3]), minus(heads[1], heads[3])
                    odd2 = quarter(odd2, 1)
                    results = (plus(even, even2), plus(odd, odd2), minus(even, even2), minus(odd, odd2))
                    for b1, (re, im) in enumerate(results):
                        b = b0 + 4 * b1
                        if b:
                            c = twist_ref[0, b : b + 1, lanes]
                            s = twist_ref[1, b : b + 1, lanes]
                            re, im = re * c - im * s, re * s + im * c
                        rows = pl.ds(k * LANES + at, 16)
                        mixed_ref[b, half, rows, :] = re.astype(jnp.bfloat16)
                        mixed_ref[b, 2 + half, rows, :] = im.astype(jnp.bfloat16)

    def spectrum(b, full_ref):
        mixed = jnp.concatenate([mixed_ref[b, part] for part in range(4)], axis=1)
        full_ref[...] = jnp.dot(mixed, weight_ref[...], preferred_element_type=jnp.float32)

    def screen(b, full_ref):
        square = line_ref[0, pl.ds(b, 1), :] - side_ref[0]
        angle = line_ref[1, pl.ds(b, 1), :] + side_ref[1]
        drop = square * lax.rsqrt(square) - 1.0
        picture = None
        for k in range(held):
            rows = slice(k * LANES, (k + 1) * LANES)
            cos_s, sin_s = turn(w_ref[k : k + 1, :] * drop + angle, SHORT_COS, SHORT_SIN)
            value = cos_s * full_ref[rows, :width] - sin_s * full_ref[rows, width:]
            picture = value if picture is None else picture + value
        picture = (picture * (line_ref[2, pl.ds(b, 1), :] * side_ref[2])).T
        send_ref[step, b] = picture[:own]
        own_ref[0, b] = picture[own : 2 * own]

    def copy(index, piece):
        lines = pl.ds(piece * PIECE, PIECE)
        return pltpu.make_async_remote_copy(
            src_ref=send_ref.at[index, lines],
            dst_ref=got_ref.at[index, lines],
            send_sem=send_sem.at[index, piece],
            recv_sem=got_sem.at[index, piece],
            device_id={"plane": partner},
            device_id_type=MESH,
        )

    spectrum(0, even_ref)

    @pl.loop(0, DIGITS // PIECE)
    def _(piece):
        for pair in range(PIECE // 2):
            b = piece * PIECE + pair * 2
            spectrum(b + 1, odd_ref)
            screen(b, even_ref)
            spectrum(lax.rem(b + 2, DIGITS), even_ref)
            screen(b + 1, odd_ref)
        copy(step, piece).start()

    @pl.when(step == steps - 1)
    def _():
        for index in range(send_ref.shape[0]):
            for piece in range(DIGITS // PIECE):
                copy(index, piece).wait()


def sum_kernel(own_ref, got_ref, out_ref):
    for b in range(DIGITS):
        out_ref[:, b, :] = own_ref[0, b] + got_ref[0, b]


def local(visibility, target, offset, taps, w_plane):
    tiles = lax.axis_size("tile")
    planes = lax.axis_size("plane")
    devices = tiles * planes
    vis_dev = visibility.shape[1]
    capacity = 2 * vis_dev // devices
    slots = devices * capacity
    blocks = slots // LANES
    band = G // tiles
    columns = G // tiles
    windows = band // WINDOW
    own = G // planes // DIGITS
    width = max(LANES, 2 * own)
    held = planes // 2
    assert windows in (1, 2)
    vmem = pl.BlockSpec(memory_space=pltpu.VMEM)
    smem = pl.BlockSpec(memory_space=pltpu.SMEM)

    numbers = range(planes)
    jumps = [[d for d in numbers if not d & bit] for bit in (1, 2)]
    gathered, level = pl.pallas_call(
        functools.partial(front_kernel, windows, tiles, jumps),
        out_shape=[
            jax.ShapeDtypeStruct((tiles, 3, blocks, LANES), jnp.float32),
            jax.ShapeDtypeStruct((held, LANES), jnp.float32),
        ],
        in_specs=[vmem] * 3 + [smem],
        out_specs=[vmem] * 2,
        scratch_shapes=[
            pltpu.VMEM((9 * devices, vis_dev), jnp.bfloat16),
            pltpu.VMEM((LANES, vis_dev), jnp.bfloat16),
            pltpu.VMEM((9 * blocks, devices * LANES), jnp.bfloat16),
            pltpu.VMEM((LANES, devices * LANES), jnp.bfloat16),
            pltpu.VMEM((devices, 4, LANES), jnp.float32),
            pltpu.VMEM((devices, 4, LANES), jnp.float32),
            pltpu.VMEM((tiles, 3, blocks, LANES), jnp.float32),
            pltpu.SemaphoreType.DMA((devices,)),
            pltpu.SemaphoreType.DMA((devices,)),
            pltpu.SemaphoreType.DMA((tiles,)),
            pltpu.SemaphoreType.DMA((tiles,)),
        ],
        compiler_params=pltpu.CompilerParams(collective_id=1, has_side_effects=True),
    )(
        visibility.reshape(2, -1, LANES),
        target.reshape(-1, LANES),
        offset.reshape(-1, LANES),
        w_plane,
    )

    first = (lax.axis_index("tile") * columns).astype(jnp.int32)
    lists = [gathered]
    for k in range(1, held):
        moves = []
        for q in range(planes):
            for t in range(tiles):
                moves.append((q * tiles + t, (q ^ jumps[t % 2][k]) * tiles + t))
        lists.append(lax.ppermute(gathered, ("plane", "tile"), moves))

    def transform(slots_of):
        line = jnp.floor((slots_of[:, 2] - 1.0) * (1.0 / G))
        counts = jnp.stack(
            [
                jnp.sum(
                    ((line >= w * WINDOW) & (line < (w + 1) * WINDOW)).astype(jnp.int32),
                    axis=(1, 2),
                )
                for w in range(windows)
            ],
            axis=1,
        )
        return pl.pallas_call(
            functools.partial(grid_kernel, windows, columns),
            grid=(tiles, windows),
            out_shape=jax.ShapeDtypeStruct((DIGITS, 2 * columns, WINDOW), jnp.float32),
            in_specs=[
                smem,
                smem,
                pl.BlockSpec((1, 3, blocks, LANES), lambda t, w: (t, 0, 0, 0)),
            ],
            out_specs=pl.BlockSpec(
                (1, 2 * columns, WINDOW), lambda t, w: (t * windows + w, 0, 0)
            ),
            scratch_shapes=[
                pltpu.VMEM((WIDE // LANES, 2 * columns, LANES), jnp.bfloat16),
                pltpu.VMEM((WIDE // LANES, WINDOW, LANES), jnp.bfloat16),
                pltpu.VMEM((2, BLOCK, WIDE), jnp.float32),
                pltpu.VMEM((2, 8, WIDE), jnp.float32),
            ],
            cost_estimate=pl.CostEstimate(
                flops=2 * slots * tiles * columns * WINDOW, bytes_accessed=1 << 24, transcendentals=0
            ),
        )(counts, first[None], slots_of).reshape(DIGITS, 2, columns, WINDOW)

    grids = [transform(v) for v in lists]

    digits = np.arange(DIGITS)
    angles = 2.0 * np.pi * (digits[:, None] * np.arange(WINDOW)[None, :]) / G
    twist = jnp.asarray(np.stack([np.cos(angles), np.sin(angles)]).astype(np.float32))
    steps = columns // LANES
    mine_part, other_part = pl.pallas_call(
        functools.partial(image_kernel, held, own, columns, 1.0 / math.sqrt(vis_dev * devices)),
        grid=(steps,),
        out_shape=[jax.ShapeDtypeStruct((steps, DIGITS, own, LANES), jnp.float32)] * 2,
        in_specs=[
            smem,
            vmem,
            vmem,
        ]
        + [pl.BlockSpec((DIGITS, 2, LANES, WINDOW), lambda j: (0, 0, j, 0))] * held,
        out_specs=[
            pl.BlockSpec((1, DIGITS, own, LANES), lambda j: (j, 0, 0, 0)),
            pl.BlockSpec(memory_space=pl.ANY),
        ],
        scratch_shapes=[
            pltpu.VMEM((DIGITS, 4, held * LANES, LANES), jnp.bfloat16),
            pltpu.VMEM((held * LANES, 2 * width), jnp.float32),
            pltpu.VMEM((held * LANES, 2 * width), jnp.float32),
            pltpu.VMEM((steps, DIGITS, own, LANES), jnp.float32),
            pltpu.VMEM((2 * WINDOW, 2 * width), jnp.bfloat16),
            pltpu.VMEM((3, DIGITS, width), jnp.float32),
            pltpu.VMEM((3, LANES, LANES), jnp.float32),
            pltpu.SemaphoreType.DMA((steps, DIGITS // PIECE)),
            pltpu.SemaphoreType.DMA((steps, DIGITS // PIECE)),
        ],
        compiler_params=pltpu.CompilerParams(
            collective_id=0,
            has_side_effects=True,
            vmem_limit_bytes=60 * 1024 * 1024,
            dimension_semantics=("arbitrary",),
        ),
    )(taps, level, twist, *grids)
    block = pl.BlockSpec((1, DIGITS, own, LANES), lambda j: (j, 0, 0, 0))
    image = pl.pallas_call(
        sum_kernel,
        grid=(steps,),
        out_shape=jax.ShapeDtypeStruct((own, DIGITS, columns), jnp.float32),
        in_specs=[block, block],
        out_specs=pl.BlockSpec((own, DIGITS, LANES), lambda j: (0, 0, j)),
    )(mine_part, other_part)
    return image.reshape(own * DIGITS, columns)


def solution(mesh):
    return jax.shard_map(
        local,
        mesh=mesh,
        in_specs=(
            P(None, ("plane", "tile")),
            P(("plane", "tile"), None),
            P(("plane", "tile")),
            P(),
            P("plane"),
        ),
        out_specs=P("plane", "tile"),
        check_vma=False,
    )
```

```python
import functools
import math

import jax
import jax.numpy as jnp
import numpy as np
from jax import lax
from jax.experimental import pallas as pl
from jax.experimental.pallas import tpu as pltpu
from jax.sharding import PartitionSpec as P

G = 4096
LANES = 128
WINDOW = 256
DIGITS = G // WINDOW
BLOCK = 64
PIECE = 4
WIDE = 1024
HALF = 512
NARROW = 256
MESH = pl.DeviceIdType.MESH


def fitted(function, terms):
    nodes = np.cos((np.arange(400) + 0.5) * np.pi / 400)
    square = 0.125 * (nodes + 1.0)
    table = np.polynomial.chebyshev.Chebyshev.fit(
        square, function(np.sqrt(square)), terms - 1, domain=[0.0, 0.25]
    )
    return [float(v) for v in table.convert(kind=np.polynomial.Polynomial).coef]


COS_COEF = fitted(lambda x: np.cos(2.0 * np.pi * x), 7)
SIN_COEF = fitted(lambda x: np.sin(2.0 * np.pi * x) / x, 6)


SHORT_COS = fitted(lambda x: np.cos(2.0 * np.pi * x), 6)
SHORT_SIN = fitted(lambda x: np.sin(2.0 * np.pi * x) / x, 5)


def horner(coefficients, x):
    total = coefficients[-1]
    for value in coefficients[-2::-1]:
        total = total * x + value
    return total


def turn(cycles, cos_terms=COS_COEF, sin_terms=SIN_COEF):
    part = cycles - jnp.round(cycles)
    square = part * part
    return horner(cos_terms, square), part * horner(sin_terms, square)


def pieces(value):
    high = value.astype(jnp.bfloat16).astype(jnp.float32)
    rest = value - high
    middle = rest.astype(jnp.bfloat16).astype(jnp.float32)
    return high, middle, rest - middle


def strict_upper(n):
    return jnp.where(
        lax.broadcasted_iota(jnp.int32, (n, n), 0) < lax.broadcasted_iota(jnp.int32, (n, n), 1),
        1.0,
        0.0,
    ).astype(jnp.bfloat16)


NT = (((1,), (1,)), ((), ()))


def flip(value, bits):
    bit = 1
    while bit <= bits:
        if bits & bit:
            value = value + bit - 2 * bit * lax.rem(value // bit, 2)
        bit *= 2
    return value


def front_kernel(
    windows, tiles, jumps, vis_ref, target_ref, offset_ref, w_ref, out_ref, level_ref,
    lhs_ref, rhs_ref, left_ref, right_ref, send_ref, got_ref, ring_ref,
    send_sem, got_sem, pass_sem, ring_sem,
):
    devices = send_ref.shape[0]
    plane, tile = lax.axis_index("plane"), lax.axis_index("tile")
    mine = plane * tiles + tile
    barrier = pltpu.get_barrier_semaphore()

    def seat(device):
        return {"plane": device // tiles, "tile": lax.rem(device, tiles)}

    @pl.loop(1, devices)
    def _(i):
        pl.semaphore_signal(
            barrier, inc=1, device_id=seat(lax.rem(mine + i, devices)), device_id_type=MESH
        )

    blocks = target_ref.shape[0]
    upper = strict_upper(LANES)
    line = lax.broadcasted_iota(jnp.int32, (devices, LANES), 0)
    slot = lax.broadcasted_iota(jnp.int32, (LANES, LANES), 0).astype(jnp.float32)
    carry = jnp.zeros((devices, 1), jnp.float32)
    for k in range(blocks):
        part = slice(k * LANES, (k + 1) * LANES)
        hit = line == target_ref[k : k + 1, :]
        hot = jnp.where(hit, 1.0, 0.0)
        before = jnp.dot(hot.astype(jnp.bfloat16), upper, preferred_element_type=jnp.float32)
        rank = jnp.sum(hot * (before + carry), axis=0, keepdims=True)
        carry = carry + jnp.sum(hot, axis=1, keepdims=True)
        rhs_ref[:, part] = jnp.where(slot == rank, 1.0, 0.0).astype(jnp.bfloat16)
        rows = (
            vis_ref[0:1, part],
            vis_ref[1:2, part],
            offset_ref[k : k + 1, :].astype(jnp.float32) + 1.0,
        )
        for p, row in enumerate(rows):
            for n, value in enumerate(pieces(row)):
                at = (p * 3 + n) * devices
                lhs_ref[at : at + devices, part] = jnp.where(hit, value, 0.0).astype(jnp.bfloat16)
    total = lax.dot_general(lhs_ref[...], rhs_ref[...], NT, preferred_element_type=jnp.float32)
    for p in range(3):
        at = p * 3 * devices
        send_ref[:, p, :] = (
            total[at : at + devices]
            + total[at + devices : at + 2 * devices]
            + total[at + 2 * devices : at + 3 * devices]
        )
    send_ref[:, 3, :] = jnp.full((devices, LANES), w_ref[0], jnp.float32)
    got_ref[mine] = send_ref[mine]
    pl.semaphore_wait(barrier, devices - 1)

    def post(source, target):
        return pltpu.make_async_remote_copy(
            src_ref=send_ref.at[target],
            dst_ref=got_ref.at[source],
            send_sem=send_sem.at[target],
            recv_sem=got_sem.at[source],
            device_id=seat(target),
            device_id_type=MESH,
        )

    @pl.loop(1, devices)
    def _(i):
        post(mine, lax.rem(mine + i, devices)).start()

    @pl.loop(1, devices)
    def _(i):
        post(lax.rem(mine + devices - i, devices), mine).wait_recv()

    for k in range(level_ref.shape[0]):
        near, far = flip(plane, jumps[0][k]), flip(plane, jumps[1][k])
        core = lax.rem(tile, 2)
        origin = (near * (1 - core) + far * core) * tiles + tile
        level_ref[k : k + 1, :] = got_ref[origin, 3:4, :]

    rows = left_ref.shape[0] // 9
    encoded = got_ref[:, 2, :]
    row = jnp.floor((encoded - 1.0) * (1.0 / G))
    lower = jnp.where(
        lax.broadcasted_iota(jnp.int32, (devices, devices), 0)
        > lax.broadcasted_iota(jnp.int32, (devices, devices), 1),
        1.0,
        0.0,
    ).astype(jnp.bfloat16)
    position = jnp.full(row.shape, -1.0, jnp.float32)
    for w in range(windows):
        member = jnp.where((row >= w * WINDOW) & (row < (w + 1) * WINDOW), 1.0, 0.0)
        flags = member.astype(jnp.bfloat16)
        inside = jnp.dot(flags, upper, preferred_element_type=jnp.float32)
        ahead = jnp.sum(
            jnp.dot(lower, flags, preferred_element_type=jnp.float32), axis=1, keepdims=True
        )
        place = inside + ahead
        number = jnp.sum(jnp.sum(member, axis=1, keepdims=True), axis=0, keepdims=True)
        ring_ref[tile, 3 * rows + w : 3 * rows + w + 1] = jnp.broadcast_to(number, (1, LANES))
        if w == 1:
            place = rows * LANES - 1 - place
        position = jnp.where(member > 0.0, place, position)
    high = jnp.floor(position * (1.0 / LANES))
    low = position - high * LANES
    line = lax.broadcasted_iota(jnp.int32, (rows, LANES), 0).astype(jnp.float32)
    parts = [pieces(got_ref[:, 0, :]), pieces(got_ref[:, 1, :]), pieces(encoded)]
    for k in range(devices):
        part = slice(k * LANES, (k + 1) * LANES)
        hit = line == high[k : k + 1, :]
        right_ref[:, part] = jnp.where(slot == low[k : k + 1, :], 1.0, 0.0).astype(jnp.bfloat16)
        for p in range(3):
            for n in range(3):
                at = (p * 3 + n) * rows
                left_ref[at : at + rows, part] = jnp.where(
                    hit, parts[p][n][k : k + 1, :], 0.0
                ).astype(jnp.bfloat16)
    total = lax.dot_general(left_ref[...], right_ref[...], NT, preferred_element_type=jnp.float32)
    for p in range(3):
        at = p * 3 * rows
        ring_ref[tile, p * rows : (p + 1) * rows] = (
            total[at : at + rows]
            + total[at + rows : at + 2 * rows]
            + total[at + 2 * rows : at + 3 * rows]
        )

    ring_ref[tile, 3 * rows + windows :] = jnp.zeros((8 - windows, LANES), jnp.float32)
    sister = tile + 1 - 2 * lax.rem(tile, 2)

    def hand(block, target, index):
        return pltpu.make_async_remote_copy(
            src_ref=ring_ref.at[block],
            dst_ref=ring_ref.at[block],
            send_sem=pass_sem.at[index],
            recv_sem=ring_sem.at[block],
            device_id={"tile": target},
            device_id_type=MESH,
        )

    steps = tiles // 2
    hand(tile, sister, 0).start()
    for i in range(1, steps):
        hand(tile, lax.rem(tile + 2 * i, tiles), i).start()
    for i in range(1, steps):
        block = lax.rem(tile + tiles - 2 * i, tiles)
        hand(block, sister, 0).wait_recv()
        hand(block, sister, steps + i).start()
    hand(sister, sister, 0).wait_recv()
    for i in range(1, steps):
        hand(lax.rem(sister + tiles - 2 * i, tiles), sister, 0).wait_recv()
    out_ref[...] = ring_ref[...]
    hand(tile, sister, 0).wait_send()
    for i in range(1, steps):
        hand(tile, lax.rem(tile + 2 * i, tiles), i).wait_send()
        hand(tile, sister, steps + i).wait_send()

    @pl.loop(1, devices)
    def _(i):
        post(mine, lax.rem(mine + i, devices)).wait_send()


def spread(re, im, leads_cos, leads_sin):
    half = len(leads_cos)
    low, high = [], []
    for cos_l, sin_l in zip(leads_cos, leads_sin):
        a, b = re * cos_l, im * sin_l
        c, d = im * cos_l, re * sin_l
        high.append((a - b, c + d))
        low.append((a + b, c - d))
    assert len(low) == half
    return low[::-1] + high


def grid_kernel(
    windows, columns, vis_ref, grid_ref, table_ref, hot_ref, near_ref, lead_ref, sum_ref, done_sem
):
    tiles = vis_ref.shape[0]
    blocks = (vis_ref.shape[1] - 8) // 3
    tops = columns // BLOCK
    base = lax.axis_index("tile") * columns + (tops - 1) * (BLOCK // 2) + 28
    eight = lax.broadcasted_iota(jnp.int32, (8, LANES), 0)
    start_at = (eight + base).astype(jnp.float32)
    lead_at = jnp.where(eight < 4, 4 + 8 * eight, 32 + 64 * (eight - 4)).astype(jnp.float32)
    lane = lax.broadcasted_iota(jnp.int32, (WINDOW, LANES), 0).astype(jnp.float32)

    def drain(item):
        slot = lax.rem(item, 2)
        return pltpu.make_async_copy(sum_ref.at[slot], grid_ref.at[item], done_sem.at[slot])

    @pl.loop(0, tiles * windows)
    def _(item):
        tile, window = item // windows, lax.rem(item, windows)

        @pl.when(item >= 2)
        def _():
            drain(item - 2).wait()

        fill(tile, window, blocks, tops, columns, start_at, lead_at, lane,
             vis_ref, sum_ref.at[lax.rem(item, 2)], table_ref, hot_ref, near_ref, lead_ref)
        drain(item).start()

    for item in range(max(0, tiles * windows - 2), tiles * windows):
        drain(item).wait()


def fill(
    tile, window, blocks, tops, columns, start_at, lead_at, lane,
    vis_ref, out_ref, table_ref, hot_ref, near_ref, lead_ref,
):
    number = vis_ref[tile, pl.ds(3 * blocks + window, 1), :][0, 0].astype(jnp.int32)
    lowest = (window * WINDOW).astype(jnp.float32)

    def build(group, row):
        part = slice(group * LANES, (group + 1) * LANES)
        vis_re = vis_ref[tile, pl.ds(row, 1), :]
        vis_im = vis_ref[tile, pl.ds(blocks + row, 1), :]
        encoded = vis_ref[tile, pl.ds(2 * blocks + row, 1), :] - 1.0
        line = jnp.floor(encoded * (1.0 / G))
        unit = (encoded - line * G) * (1.0 / G)
        hot_ref[group, :WINDOW] = jnp.where(lane == line - lowest, 1.0, 0.0).astype(jnp.bfloat16)
        start_cos, start_sin = turn(start_at * unit)
        lead_cos, lead_sin = turn(lead_at * unit)
        first_re = vis_re * start_cos - vis_im * start_sin
        first_im = vis_re * start_sin + vis_im * start_cos
        small = spread(
            first_re,
            first_im,
            [lead_cos[i : i + 1] for i in range(4)],
            [lead_sin[i : i + 1] for i in range(4)],
        )
        for i, (re, im) in enumerate(small):
            near_ref[0, 8 * i : 8 * i + 8, part] = re
            near_ref[1, 8 * i : 8 * i + 8, part] = im
        lead_ref[0, :, part] = lead_cos
        lead_ref[1, :, part] = lead_sin

    def widen(group):
        part = slice(group * LANES, (group + 1) * LANES)
        for i in range(tops // 2):
            cos_l = lead_ref[0, 4 + i : 5 + i, part]
            sin_l = lead_ref[1, 4 + i : 5 + i, part]
            for lines in range(0, BLOCK, 16):
                re = near_ref[0, lines : lines + 16, part]
                im = near_ref[1, lines : lines + 16, part]
                a, b = re * cos_l, im * sin_l
                c, d = im * cos_l, re * sin_l
                at = (i * BLOCK + lines) * 4
                for n, value in enumerate((a - b, a + b, c + d, c - d)):
                    table_ref[group, at + 16 * n : at + 16 * n + 16, :] = value.astype(
                        jnp.bfloat16
                    )

    def deliver(product, add):
        for i in range(tops // 2):
            for lines in range(0, BLOCK, 16):
                high = (tops // 2 + i) * BLOCK + lines
                low = (tops // 2 - 1 - i) * BLOCK + lines
                at = (i * BLOCK + lines) * 4
                for n, row in enumerate((high, low, columns + high, columns + low)):
                    value = product[at + 16 * n : at + 16 * n + 16]
                    if add:
                        value = value + out_ref[row : row + 16]
                    out_ref[row : row + 16] = value

    def chunk(row, width, add):
        for group in range(width // LANES):
            build(group, row + group)
        for group in range(width // LANES):
            widen(group)
        groups = range(width // LANES)
        left = jnp.concatenate([table_ref[group, : 2 * columns] for group in groups], axis=1)
        right = jnp.concatenate([hot_ref[group, :WINDOW] for group in groups], axis=1)
        deliver(lax.dot_general(left, right, NT, preferred_element_type=jnp.float32), add)

    def place(done, width):
        return jnp.where(window == 0, done, blocks - done - width // LANES)

    @pl.when(number <= NARROW)
    def _():
        chunk(place(0, NARROW), NARROW, False)

    @pl.when((number > NARROW) & (number <= HALF))
    def _():
        chunk(place(0, HALF), HALF, False)

    @pl.when((number > HALF) & (number <= HALF + NARROW))
    def _():
        chunk(place(0, HALF + NARROW), HALF + NARROW, False)

    @pl.when(number > HALF + NARROW)
    def _():
        chunk(place(0, WIDE), WIDE, False)

    rest = jnp.maximum(number - WIDE, 0)
    full = rest // WIDE
    tail = rest - full * WIDE
    full = full + jnp.where(tail > HALF, 1, 0)

    @pl.loop(0, full)
    def _(index):
        chunk(place((index + 1) * (WIDE // LANES), WIDE), WIDE, True)

    done = (full + 1) * (WIDE // LANES)

    @pl.when((tail > NARROW) & (tail <= HALF))
    def _():
        chunk(place(done, HALF), HALF, True)

    @pl.when((tail > 0) & (tail <= NARROW))
    def _():
        chunk(place(done, NARROW), NARROW, True)


def place(lane, first, second, count):
    return lax.rem(jnp.where(lane < count, first * count + lane, second * count + lane - count), WINDOW)


def squared(index):
    cosine = jnp.where(index >= G // 2, index - G, index).astype(jnp.float32) * (0.5 / G)
    return cosine * cosine


def response(taps, index):
    real = imag = None
    for j, tap in enumerate(taps):
        cos_j, sin_j = turn((index * j).astype(jnp.float32) * (1.0 / G))
        real = tap * cos_j if real is None else real + tap * cos_j
        imag = tap * sin_j if imag is None else imag + tap * sin_j
    return jnp.arctan2(imag, real) * (0.5 / math.pi), jnp.sqrt(real * real + imag * imag)


def quarter(value, turns):
    re, im = value
    return ((re, im), (-im, re), (-re, -im), (im, -re))[turns % 4]


def rotate(value, sixteenths):
    value = quarter(value, sixteenths // 4)
    rest = sixteenths % 4
    if rest == 0:
        return value
    re, im = value
    if rest == 2:
        root = math.sqrt(0.5)
        return (re - im) * root, (re + im) * root
    c, s = math.cos(rest * math.pi / 8), math.sin(rest * math.pi / 8)
    return re * c - im * s, re * s + im * c


def plus(left, right):
    return left[0] + right[0], left[1] + right[1]


def minus(left, right):
    return left[0] - right[0], left[1] - right[1]


def image_kernel(held, own, columns, scale, taps_ref, w_ref, *refs):
    grids, own_ref, got_ref = refs[:held], refs[held], refs[held + 1]
    mixed_ref, even_ref, odd_ref, send_ref, weight_ref, line_ref, side_ref = refs[held + 2 : -4]
    held_ref, send_sem, got_sem, load_sem = refs[-4:]
    width = line_ref.shape[2]
    step = pl.program_id(0)
    steps = pl.num_programs(0)
    mine = lax.axis_index("plane")
    core = lax.rem(lax.axis_index("tile"), 2)
    near = mine + 1 - 2 * lax.rem(mine, 2)
    far = mine + 2 - 4 * lax.rem(mine // 2, 2)
    partner = near * (1 - core) + far * core
    barrier = pltpu.get_barrier_semaphore()

    def fetch(index, k):
        slot = lax.rem(index, 2)
        lines = pl.ds(pl.multiple_of(index * LANES, LANES), LANES)
        return pltpu.make_async_copy(
            grids[k].at[:, :, lines, :], held_ref.at[slot, k], load_sem.at[slot, k]
        )

    @pl.when(step == 0)
    def _():
        for k in range(held):
            fetch(step, k).start()

    @pl.when(step < steps - 1)
    def _():
        for k in range(held):
            fetch(step + 1, k).start()

    @pl.when(step == 0)
    def _():
        pl.semaphore_signal(
            barrier, inc=1, device_id={"plane": partner}, device_id_type=MESH
        )
        lane = lax.broadcasted_iota(jnp.int32, (DIGITS, width), 1)
        digit = lax.broadcasted_iota(jnp.int32, (DIGITS, width), 0)
        index = place(lane, partner, mine, own) * DIGITS + digit
        taps = [taps_ref[j] for j in range(taps_ref.shape[0])]
        angle, size = response(taps, index)
        line_ref[0] = 1.0 - squared(index)
        line_ref[1] = angle
        line_ref[2] = size * scale

        @pl.loop(0, WINDOW // 16)
        def _(i):
            at = pl.multiple_of(i * 16, 16)
            lane = lax.broadcasted_iota(jnp.int32, (16, width), 1)
            inner = lax.broadcasted_iota(jnp.int32, (16, width), 0) + at
            product = inner * place(lane, partner, mine, own)
            cos_d, sin_d = turn(product.astype(jnp.float32) * (1.0 / WINDOW))
            cos_s, sin_s = turn(inner.astype(jnp.float32) * (1.0 / G))
            upper, under = pl.ds(at, 16), pl.ds(WINDOW + at, 16)
            for b in range(DIGITS):
                real = cos_d.astype(jnp.bfloat16)
                weight_ref[b, 0, upper, :] = real
                weight_ref[b, 1, upper, :] = sin_d.astype(jnp.bfloat16)
                weight_ref[b, 0, under, :] = (-sin_d).astype(jnp.bfloat16)
                weight_ref[b, 1, under, :] = real
                cos_d, sin_d = cos_d * cos_s - sin_d * sin_s, cos_d * sin_s + sin_d * cos_s

        pl.semaphore_wait(barrier, 1)

    index = lax.axis_index("tile") * columns + step * LANES
    index = index + lax.broadcasted_iota(jnp.int32, (8, LANES), 1)
    taps = [
        jnp.full((8, LANES), taps_ref[j], jnp.float32).astype(jnp.bfloat16).astype(jnp.float32)
        for j in range(taps_ref.shape[0])
    ]
    angle, size = response(taps, index)
    for n, value in enumerate((squared(index), angle, size)):
        side_ref[n] = jnp.broadcast_to(value[0:1], (LANES, LANES)).T

    for k in range(held):
        fetch(step, k).wait()
        grid_ref = held_ref.at[lax.rem(step, 2), k]

        @pl.loop(0, LANES // 16)
        def _(index):
            at = pl.multiple_of(index * 16, 16)
            part = pl.ds(at, 16)
            for half in range(WINDOW // LANES):
                lanes = slice(half * LANES, (half + 1) * LANES)
                for b0 in range(4):
                    heads = []
                    for w0 in range(4):
                        total = None
                        for w1 in range(4):
                            w = 4 * w1 + w0
                            value = quarter(
                                (grid_ref[w, 0, part, lanes], grid_ref[w, 1, part, lanes]), w1 * b0
                            )
                            total = value if total is None else plus(total, value)
                        total = rotate(total, w0 * b0)
                        heads.append(total)
                    even, odd = plus(heads[0], heads[2]), minus(heads[0], heads[2])
                    even2, odd2 = plus(heads[1], heads[3]), minus(heads[1], heads[3])
                    odd2 = quarter(odd2, 1)
                    results = (plus(even, even2), plus(odd, odd2), minus(even, even2), minus(odd, odd2))
                    for b1, (re, im) in enumerate(results):
                        b = b0 + 4 * b1
                        rows = pl.ds(k * LANES + at, 16)
                        mixed_ref[b, half, rows, :] = re.astype(jnp.bfloat16)
                        mixed_ref[b, 2 + half, rows, :] = im.astype(jnp.bfloat16)

    def spectrum(b, full_ref):
        mixed = jnp.concatenate([mixed_ref[b, part] for part in range(4)], axis=1)
        weight = jnp.concatenate([weight_ref[b, part] for part in range(2)], axis=1)
        full_ref[...] = jnp.dot(mixed, weight, preferred_element_type=jnp.float32)

    def screen(b, full_ref):
        square = line_ref[0, pl.ds(b, 1), :] - side_ref[0]
        angle = line_ref[1, pl.ds(b, 1), :] + side_ref[1]
        drop = square * lax.rsqrt(square) - 1.0
        picture = None
        for k in range(held):
            rows = slice(k * LANES, (k + 1) * LANES)
            cos_s, sin_s = turn(w_ref[k : k + 1, :] * drop + angle, SHORT_COS, SHORT_SIN)
            value = cos_s * full_ref[rows, :width] - sin_s * full_ref[rows, width:]
            picture = value if picture is None else picture + value
        picture = (picture * (line_ref[2, pl.ds(b, 1), :] * side_ref[2])).T
        send_ref[step, b] = picture[:own]
        own_ref[0, b] = picture[own : 2 * own]

    def copy(index, piece):
        lines = pl.ds(piece * PIECE, PIECE)
        return pltpu.make_async_remote_copy(
            src_ref=send_ref.at[index, lines],
            dst_ref=got_ref.at[index, lines],
            send_sem=send_sem.at[index, piece],
            recv_sem=got_sem.at[index, piece],
            device_id={"plane": partner},
            device_id_type=MESH,
        )

    spectrum(0, even_ref)

    @pl.loop(0, DIGITS // PIECE)
    def _(piece):
        for pair in range(PIECE // 2):
            b = piece * PIECE + pair * 2
            spectrum(b + 1, odd_ref)
            screen(b, even_ref)
            spectrum(lax.rem(b + 2, DIGITS), even_ref)
            screen(b + 1, odd_ref)
        copy(step, piece).start()

    @pl.when(step == steps - 1)
    def _():
        for index in range(send_ref.shape[0]):
            for piece in range(DIGITS // PIECE):
                copy(index, piece).wait()


def sum_kernel(own_ref, got_ref, out_ref):
    for index in range(own_ref.shape[0]):
        lanes = slice(index * LANES, (index + 1) * LANES)
        for b in range(DIGITS):
            out_ref[:, b, lanes] = own_ref[index, b] + got_ref[index, b]


def local(visibility, target, offset, taps, w_plane):
    tiles = lax.axis_size("tile")
    planes = lax.axis_size("plane")
    devices = tiles * planes
    vis_dev = visibility.shape[1]
    capacity = 2 * vis_dev // devices
    slots = devices * capacity
    blocks = slots // LANES
    band = G // tiles
    columns = G // tiles
    windows = band // WINDOW
    own = G // planes // DIGITS
    width = max(LANES, 2 * own)
    held = planes // 2
    assert windows in (1, 2)
    vmem = pl.BlockSpec(memory_space=pltpu.VMEM)
    smem = pl.BlockSpec(memory_space=pltpu.SMEM)

    numbers = range(planes)
    jumps = [[d for d in numbers if not d & bit] for bit in (1, 2)]
    gathered, level = pl.pallas_call(
        functools.partial(front_kernel, windows, tiles, jumps),
        out_shape=[
            jax.ShapeDtypeStruct((tiles, 3 * blocks + 8, LANES), jnp.float32),
            jax.ShapeDtypeStruct((held, LANES), jnp.float32),
        ],
        in_specs=[vmem] * 3 + [smem],
        out_specs=[vmem] * 2,
        scratch_shapes=[
            pltpu.VMEM((9 * devices, vis_dev), jnp.bfloat16),
            pltpu.VMEM((LANES, vis_dev), jnp.bfloat16),
            pltpu.VMEM((9 * blocks, devices * LANES), jnp.bfloat16),
            pltpu.VMEM((LANES, devices * LANES), jnp.bfloat16),
            pltpu.VMEM((devices, 4, LANES), jnp.float32),
            pltpu.VMEM((devices, 4, LANES), jnp.float32),
            pltpu.VMEM((tiles, 3 * blocks + 8, LANES), jnp.float32),
            pltpu.SemaphoreType.DMA((devices,)),
            pltpu.SemaphoreType.DMA((devices,)),
            pltpu.SemaphoreType.DMA((tiles,)),
            pltpu.SemaphoreType.DMA((tiles,)),
        ],
        compiler_params=pltpu.CompilerParams(collective_id=1, has_side_effects=True),
    )(
        visibility,
        target.reshape(-1, LANES),
        offset.reshape(-1, LANES),
        w_plane,
    )

    lists = [gathered]
    for k in range(1, held):
        moves = []
        for q in range(planes):
            for t in range(tiles):
                moves.append((q * tiles + t, (q ^ jumps[t % 2][k]) * tiles + t))
        lists.append(lax.ppermute(gathered, ("plane", "tile"), moves))

    def transform(slots_of):
        return pl.pallas_call(
            functools.partial(grid_kernel, windows, columns),
            out_shape=jax.ShapeDtypeStruct((DIGITS, 2 * columns, WINDOW), jnp.float32),
            in_specs=[vmem],
            out_specs=pl.BlockSpec(memory_space=pl.ANY),
            scratch_shapes=[
                pltpu.VMEM((WIDE // LANES, 2 * columns + 16, LANES), jnp.bfloat16),
                pltpu.VMEM((WIDE // LANES, WINDOW + 16, LANES), jnp.bfloat16),
                pltpu.VMEM((2, BLOCK + 8, WIDE + LANES), jnp.float32),
                pltpu.VMEM((2, 8, WIDE), jnp.float32),
                pltpu.VMEM((2, 2 * columns, WINDOW), jnp.float32),
                pltpu.SemaphoreType.DMA((2,)),
            ],
            cost_estimate=pl.CostEstimate(
                flops=2 * slots * tiles * columns * WINDOW, bytes_accessed=1 << 24, transcendentals=0
            ),
        )(slots_of).reshape(DIGITS, 2, columns, WINDOW)

    grids = [transform(v) for v in lists]

    steps = columns // LANES
    mine_part, other_part = pl.pallas_call(
        functools.partial(image_kernel, held, own, columns, 1.0 / math.sqrt(vis_dev * devices)),
        grid=(steps,),
        out_shape=[jax.ShapeDtypeStruct((steps, DIGITS, own, LANES), jnp.float32)] * 2,
        in_specs=[
            smem,
            vmem,
        ]
        + [pl.BlockSpec(memory_space=pl.ANY)] * held,
        out_specs=[
            pl.BlockSpec((1, DIGITS, own, LANES), lambda j: (j, 0, 0, 0)),
            pl.BlockSpec(memory_space=pl.ANY),
        ],
        scratch_shapes=[
            pltpu.VMEM((DIGITS, 4, held * LANES, LANES), jnp.bfloat16),
            pltpu.VMEM((held * LANES, 2 * width), jnp.float32),
            pltpu.VMEM((held * LANES, 2 * width), jnp.float32),
            pltpu.VMEM((steps, DIGITS, own, LANES), jnp.float32),
            pltpu.VMEM((DIGITS, 2, 2 * WINDOW, width), jnp.bfloat16),
            pltpu.VMEM((3, DIGITS, width), jnp.float32),
            pltpu.VMEM((3, LANES, LANES), jnp.float32),
            pltpu.VMEM((2, held, DIGITS, 2, LANES, WINDOW), jnp.float32),
            pltpu.SemaphoreType.DMA((steps, DIGITS // PIECE)),
            pltpu.SemaphoreType.DMA((steps, DIGITS // PIECE)),
            pltpu.SemaphoreType.DMA((2, held)),
        ],
        compiler_params=pltpu.CompilerParams(
            collective_id=0,
            has_side_effects=True,
            vmem_limit_bytes=60 * 1024 * 1024,
            dimension_semantics=("arbitrary",),
        ),
    )(taps, level, *grids)
    block = pl.BlockSpec((steps // 2, DIGITS, own, LANES), lambda j: (j, 0, 0, 0))
    image = pl.pallas_call(
        sum_kernel,
        grid=(2,),
        out_shape=jax.ShapeDtypeStruct((own, DIGITS, columns), jnp.float32),
        in_specs=[block, block],
        out_specs=pl.BlockSpec((own, DIGITS, columns // 2), lambda j: (0, 0, j)),
    )(mine_part, other_part)
    return image.reshape(own * DIGITS, columns)


def solution(mesh):
    return jax.shard_map(
        local,
        mesh=mesh,
        in_specs=(
            P(None, ("plane", "tile")),
            P(("plane", "tile"), None),
            P(("plane", "tile")),
            P(),
            P("plane"),
        ),
        out_specs=P("plane", "tile"),
        check_vma=False,
    )
```

```python
import functools
import math

import jax
import jax.numpy as jnp
import numpy as np
from jax import lax
from jax.experimental import pallas as pl
from jax.experimental.pallas import tpu as pltpu
from jax.sharding import PartitionSpec as P

G = 4096
LANES = 128
WINDOW = 256
DIGITS = G // WINDOW
BLOCK = 64
PIECE = 4
WIDE = 1024
HALF = 512
NARROW = 256
MESH = pl.DeviceIdType.MESH


def fitted(function, terms):
    nodes = np.cos((np.arange(400) + 0.5) * np.pi / 400)
    square = 0.125 * (nodes + 1.0)
    table = np.polynomial.chebyshev.Chebyshev.fit(
        square, function(np.sqrt(square)), terms - 1, domain=[0.0, 0.25]
    )
    return [float(v) for v in table.convert(kind=np.polynomial.Polynomial).coef]


COS_COEF = fitted(lambda x: np.cos(2.0 * np.pi * x), 7)
SIN_COEF = fitted(lambda x: np.sin(2.0 * np.pi * x) / x, 6)


SHORT_COS = fitted(lambda x: np.cos(2.0 * np.pi * x), 6)
SHORT_SIN = fitted(lambda x: np.sin(2.0 * np.pi * x) / x, 5)


def horner(coefficients, x):
    total = coefficients[-1]
    for value in coefficients[-2::-1]:
        total = total * x + value
    return total


def turn(cycles, cos_terms=COS_COEF, sin_terms=SIN_COEF):
    part = cycles - jnp.round(cycles)
    square = part * part
    return horner(cos_terms, square), part * horner(sin_terms, square)


def pieces(value):
    high = value.astype(jnp.bfloat16).astype(jnp.float32)
    rest = value - high
    middle = rest.astype(jnp.bfloat16).astype(jnp.float32)
    return high, middle, rest - middle


def strict_upper(n):
    return jnp.where(
        lax.broadcasted_iota(jnp.int32, (n, n), 0) < lax.broadcasted_iota(jnp.int32, (n, n), 1),
        1.0,
        0.0,
    ).astype(jnp.bfloat16)


NT = (((1,), (1,)), ((), ()))


def flip(value, bits):
    bit = 1
    while bit <= bits:
        if bits & bit:
            value = value + bit - 2 * bit * lax.rem(value // bit, 2)
        bit *= 2
    return value


def front_kernel(
    windows, tiles, jumps, vis_in, target_in, offset_in, w_ref, out_ref, level_ref,
    vis_ref, target_ref, offset_ref, in_sem, lhs_ref, rhs_ref, left_ref, right_ref, send_ref, got_ref, ring_ref,
    send_sem, got_sem, pass_sem, ring_sem,
):
    devices = send_ref.shape[0]
    plane, tile = lax.axis_index("plane"), lax.axis_index("tile")
    mine = plane * tiles + tile
    barrier = pltpu.get_barrier_semaphore()
    inputs = [
        pltpu.make_async_copy(source, target, in_sem.at[n])
        for n, (source, target) in enumerate(
            ((vis_in, vis_ref), (target_in, target_ref), (offset_in, offset_ref))
        )
    ]
    for copy in inputs:
        copy.start()

    def seat(device):
        return {"plane": device // tiles, "tile": lax.rem(device, tiles)}

    @pl.loop(1, devices)
    def _(i):
        pl.semaphore_signal(
            barrier, inc=1, device_id=seat(lax.rem(mine + i, devices)), device_id_type=MESH
        )

    for copy in inputs:
        copy.wait()
    blocks = target_ref.shape[0]
    upper = strict_upper(LANES)
    line = lax.broadcasted_iota(jnp.int32, (devices, LANES), 0)
    slot = lax.broadcasted_iota(jnp.int32, (LANES, LANES), 0).astype(jnp.float32)
    carry = jnp.zeros((devices, 1), jnp.float32)
    for k in range(blocks):
        part = slice(k * LANES, (k + 1) * LANES)
        hit = line == target_ref[k : k + 1, :]
        hot = jnp.where(hit, 1.0, 0.0)
        before = jnp.dot(hot.astype(jnp.bfloat16), upper, preferred_element_type=jnp.float32)
        rank = jnp.sum(hot * (before + carry), axis=0, keepdims=True)
        carry = carry + jnp.sum(hot, axis=1, keepdims=True)
        rhs_ref[:, part] = jnp.where(slot == rank, 1.0, 0.0).astype(jnp.bfloat16)
        rows = (
            vis_ref[0:1, part],
            vis_ref[1:2, part],
            offset_ref[k : k + 1, :].astype(jnp.float32) + 1.0,
        )
        for p, row in enumerate(rows):
            for n, value in enumerate(pieces(row)):
                at = (p * 3 + n) * devices
                lhs_ref[at : at + devices, part] = jnp.where(hit, value, 0.0).astype(jnp.bfloat16)
    total = lax.dot_general(lhs_ref[...], rhs_ref[...], NT, preferred_element_type=jnp.float32)
    for p in range(3):
        at = p * 3 * devices
        send_ref[:, p, :] = (
            total[at : at + devices]
            + total[at + devices : at + 2 * devices]
            + total[at + 2 * devices : at + 3 * devices]
        )
    send_ref[:, 3, :] = jnp.full((devices, LANES), w_ref[0], jnp.float32)
    got_ref[mine] = send_ref[mine]
    pl.semaphore_wait(barrier, devices - 1)

    def post(source, target):
        return pltpu.make_async_remote_copy(
            src_ref=send_ref.at[target],
            dst_ref=got_ref.at[source],
            send_sem=send_sem.at[target],
            recv_sem=got_sem.at[source],
            device_id=seat(target),
            device_id_type=MESH,
        )

    @pl.loop(1, devices)
    def _(i):
        post(mine, lax.rem(mine + i, devices)).start()

    @pl.loop(1, devices)
    def _(i):
        post(lax.rem(mine + devices - i, devices), mine).wait_recv()

    for k in range(level_ref.shape[0]):
        near, far = flip(plane, jumps[0][k]), flip(plane, jumps[1][k])
        core = lax.rem(tile, 2)
        origin = (near * (1 - core) + far * core) * tiles + tile
        level_ref[k : k + 1, :] = got_ref[origin, 3:4, :]

    rows = left_ref.shape[0] // 9
    encoded = got_ref[:, 2, :]
    row = jnp.floor((encoded - 1.0) * (1.0 / G))
    lower = jnp.where(
        lax.broadcasted_iota(jnp.int32, (devices, devices), 0)
        > lax.broadcasted_iota(jnp.int32, (devices, devices), 1),
        1.0,
        0.0,
    ).astype(jnp.bfloat16)
    position = jnp.full(row.shape, -1.0, jnp.float32)
    for w in range(windows):
        member = jnp.where((row >= w * WINDOW) & (row < (w + 1) * WINDOW), 1.0, 0.0)
        flags = member.astype(jnp.bfloat16)
        inside = jnp.dot(flags, upper, preferred_element_type=jnp.float32)
        ahead = jnp.sum(
            jnp.dot(lower, flags, preferred_element_type=jnp.float32), axis=1, keepdims=True
        )
        place = inside + ahead
        number = jnp.sum(jnp.sum(member, axis=1, keepdims=True), axis=0, keepdims=True)
        ring_ref[tile, 3 * rows + w : 3 * rows + w + 1] = jnp.broadcast_to(number, (1, LANES))
        if w == 1:
            place = rows * LANES - 1 - place
        position = jnp.where(member > 0.0, place, position)
    high = jnp.floor(position * (1.0 / LANES))
    low = position - high * LANES
    line = lax.broadcasted_iota(jnp.int32, (rows, LANES), 0).astype(jnp.float32)
    parts = [pieces(got_ref[:, 0, :]), pieces(got_ref[:, 1, :]), pieces(encoded)]
    for k in range(devices):
        part = slice(k * LANES, (k + 1) * LANES)
        hit = line == high[k : k + 1, :]
        right_ref[:, part] = jnp.where(slot == low[k : k + 1, :], 1.0, 0.0).astype(jnp.bfloat16)
        for p in range(3):
            for n in range(3):
                at = (p * 3 + n) * rows
                left_ref[at : at + rows, part] = jnp.where(
                    hit, parts[p][n][k : k + 1, :], 0.0
                ).astype(jnp.bfloat16)
    total = lax.dot_general(left_ref[...], right_ref[...], NT, preferred_element_type=jnp.float32)
    for p in range(3):
        at = p * 3 * rows
        ring_ref[tile, p * rows : (p + 1) * rows] = (
            total[at : at + rows]
            + total[at + rows : at + 2 * rows]
            + total[at + 2 * rows : at + 3 * rows]
        )

    ring_ref[tile, 3 * rows + windows :] = jnp.zeros((8 - windows, LANES), jnp.float32)
    sister = tile + 1 - 2 * lax.rem(tile, 2)

    def hand(block, target, index):
        return pltpu.make_async_remote_copy(
            src_ref=ring_ref.at[block],
            dst_ref=ring_ref.at[block],
            send_sem=pass_sem.at[index],
            recv_sem=ring_sem.at[block],
            device_id={"tile": target},
            device_id_type=MESH,
        )

    steps = tiles // 2
    hand(tile, sister, 0).start()
    for i in range(1, steps):
        hand(tile, lax.rem(tile + 2 * i, tiles), i).start()
    for i in range(1, steps):
        block = lax.rem(tile + tiles - 2 * i, tiles)
        hand(block, sister, 0).wait_recv()
        hand(block, sister, steps + i).start()
    hand(sister, sister, 0).wait_recv()
    for i in range(1, steps):
        hand(lax.rem(sister + tiles - 2 * i, tiles), sister, 0).wait_recv()
    out_ref[...] = ring_ref[...]
    hand(tile, sister, 0).wait_send()
    for i in range(1, steps):
        hand(tile, lax.rem(tile + 2 * i, tiles), i).wait_send()
        hand(tile, sister, steps + i).wait_send()

    @pl.loop(1, devices)
    def _(i):
        post(mine, lax.rem(mine + i, devices)).wait_send()


def spread(re, im, leads_cos, leads_sin):
    half = len(leads_cos)
    low, high = [], []
    for cos_l, sin_l in zip(leads_cos, leads_sin):
        a, b = re * cos_l, im * sin_l
        c, d = im * cos_l, re * sin_l
        high.append((a - b, c + d))
        low.append((a + b, c - d))
    assert len(low) == half
    return low[::-1] + high


def grid_kernel(
    windows, columns, list_ref, grid_ref, table_ref, hot_ref, near_ref, lead_ref, sum_ref, vis_ref,
    done_sem, load_sem,
):
    tiles = vis_ref.shape[0]

    def load(tile):
        return pltpu.make_async_copy(list_ref.at[tile], vis_ref.at[tile], load_sem.at[tile])

    @pl.loop(0, tiles)
    def _(tile):
        load(tile).start()

    blocks = (vis_ref.shape[1] - 8) // 3
    tops = columns // BLOCK
    base = lax.axis_index("tile") * columns + (tops - 1) * (BLOCK // 2) + 28
    eight = lax.broadcasted_iota(jnp.int32, (8, LANES), 0)
    start_at = (eight + base).astype(jnp.float32)
    lead_at = jnp.where(eight < 4, 4 + 8 * eight, 32 + 64 * (eight - 4)).astype(jnp.float32)
    lane = lax.broadcasted_iota(jnp.int32, (WINDOW, LANES), 0).astype(jnp.float32)

    def drain(item):
        slot = lax.rem(item, 2)
        return pltpu.make_async_copy(sum_ref.at[slot], grid_ref.at[item], done_sem.at[slot])

    @pl.loop(0, tiles * windows)
    def _(item):
        tile, window = item // windows, lax.rem(item, windows)

        @pl.when(window == 0)
        def _():
            load(tile).wait()

        @pl.when(item >= 2)
        def _():
            drain(item - 2).wait()

        fill(tile, window, blocks, tops, columns, start_at, lead_at, lane,
             vis_ref, sum_ref.at[lax.rem(item, 2)], table_ref, hot_ref, near_ref, lead_ref)
        drain(item).start()

    for item in range(max(0, tiles * windows - 2), tiles * windows):
        drain(item).wait()


def fill(
    tile, window, blocks, tops, columns, start_at, lead_at, lane,
    vis_ref, out_ref, table_ref, hot_ref, near_ref, lead_ref,
):
    number = vis_ref[tile, pl.ds(3 * blocks + window, 1), :][0, 0].astype(jnp.int32)
    lowest = (window * WINDOW).astype(jnp.float32)

    def build(group, row):
        part = slice(group * LANES, (group + 1) * LANES)
        vis_re = vis_ref[tile, pl.ds(row, 1), :]
        vis_im = vis_ref[tile, pl.ds(blocks + row, 1), :]
        encoded = vis_ref[tile, pl.ds(2 * blocks + row, 1), :] - 1.0
        line = jnp.floor(encoded * (1.0 / G))
        unit = (encoded - line * G) * (1.0 / G)
        hot_ref[group, :WINDOW] = jnp.where(lane == line - lowest, 1.0, 0.0).astype(jnp.bfloat16)
        start_cos, start_sin = turn(start_at * unit)
        lead_cos, lead_sin = turn(lead_at * unit)
        first_re = vis_re * start_cos - vis_im * start_sin
        first_im = vis_re * start_sin + vis_im * start_cos
        small = spread(
            first_re,
            first_im,
            [lead_cos[i : i + 1] for i in range(4)],
            [lead_sin[i : i + 1] for i in range(4)],
        )
        for i, (re, im) in enumerate(small):
            near_ref[0, 8 * i : 8 * i + 8, part] = re
            near_ref[1, 8 * i : 8 * i + 8, part] = im
        lead_ref[0, :, part] = lead_cos
        lead_ref[1, :, part] = lead_sin

    def widen(group):
        part = slice(group * LANES, (group + 1) * LANES)
        for i in range(tops // 2):
            cos_l = lead_ref[0, 4 + i : 5 + i, part]
            sin_l = lead_ref[1, 4 + i : 5 + i, part]
            for lines in range(0, BLOCK, 16):
                re = near_ref[0, lines : lines + 16, part]
                im = near_ref[1, lines : lines + 16, part]
                a, b = re * cos_l, im * sin_l
                c, d = im * cos_l, re * sin_l
                at = (i * BLOCK + lines) * 4
                for n, value in enumerate((a - b, a + b, c + d, c - d)):
                    table_ref[group, at + 16 * n : at + 16 * n + 16, :] = value.astype(
                        jnp.bfloat16
                    )

    def deliver(product, add):
        for i in range(tops // 2):
            for lines in range(0, BLOCK, 16):
                high = (tops // 2 + i) * BLOCK + lines
                low = (tops // 2 - 1 - i) * BLOCK + lines
                at = (i * BLOCK + lines) * 4
                for n, row in enumerate((high, low, columns + high, columns + low)):
                    value = product[at + 16 * n : at + 16 * n + 16]
                    if add:
                        value = value + out_ref[row : row + 16]
                    out_ref[row : row + 16] = value

    def chunk(row, width, add):
        for group in range(width // LANES):
            build(group, row + group)
        for group in range(width // LANES):
            widen(group)
        groups = range(width // LANES)
        left = jnp.concatenate([table_ref[group, : 2 * columns] for group in groups], axis=1)
        right = jnp.concatenate([hot_ref[group, :WINDOW] for group in groups], axis=1)
        deliver(lax.dot_general(left, right, NT, preferred_element_type=jnp.float32), add)

    def place(done, width):
        return jnp.where(window == 0, done, blocks - done - width // LANES)

    @pl.when(number <= NARROW)
    def _():
        chunk(place(0, NARROW), NARROW, False)

    @pl.when((number > NARROW) & (number <= HALF))
    def _():
        chunk(place(0, HALF), HALF, False)

    @pl.when((number > HALF) & (number <= HALF + NARROW))
    def _():
        chunk(place(0, HALF + NARROW), HALF + NARROW, False)

    @pl.when(number > HALF + NARROW)
    def _():
        chunk(place(0, WIDE), WIDE, False)

    rest = jnp.maximum(number - WIDE, 0)
    full = rest // WIDE
    tail = rest - full * WIDE
    full = full + jnp.where(tail > HALF, 1, 0)

    @pl.loop(0, full)
    def _(index):
        chunk(place((index + 1) * (WIDE // LANES), WIDE), WIDE, True)

    done = (full + 1) * (WIDE // LANES)

    @pl.when((tail > NARROW) & (tail <= HALF))
    def _():
        chunk(place(done, HALF), HALF, True)

    @pl.when((tail > 0) & (tail <= NARROW))
    def _():
        chunk(place(done, NARROW), NARROW, True)


def place(lane, first, second, count):
    return lax.rem(jnp.where(lane < count, first * count + lane, second * count + lane - count), WINDOW)


def squared(index):
    cosine = jnp.where(index >= G // 2, index - G, index).astype(jnp.float32) * (0.5 / G)
    return cosine * cosine


def response(taps, index):
    real = imag = None
    for j, tap in enumerate(taps):
        cos_j, sin_j = turn((index * j).astype(jnp.float32) * (1.0 / G))
        real = tap * cos_j if real is None else real + tap * cos_j
        imag = tap * sin_j if imag is None else imag + tap * sin_j
    return jnp.arctan2(imag, real) * (0.5 / math.pi), jnp.sqrt(real * real + imag * imag)


def quarter(value, turns):
    re, im = value
    return ((re, im), (-im, re), (-re, -im), (im, -re))[turns % 4]


def rotate(value, sixteenths):
    value = quarter(value, sixteenths // 4)
    rest = sixteenths % 4
    if rest == 0:
        return value
    re, im = value
    if rest == 2:
        root = math.sqrt(0.5)
        return (re - im) * root, (re + im) * root
    c, s = math.cos(rest * math.pi / 8), math.sin(rest * math.pi / 8)
    return re * c - im * s, re * s + im * c


def plus(left, right):
    return left[0] + right[0], left[1] + right[1]


def minus(left, right):
    return left[0] - right[0], left[1] - right[1]


def image_kernel(held, own, columns, scale, taps_ref, w_ref, *refs):
    grids, own_ref, got_ref = refs[:held], refs[held], refs[held + 1]
    mixed_ref, even_ref, odd_ref, send_ref, weight_ref, line_ref, side_ref = refs[held + 2 : -4]
    held_ref, send_sem, got_sem, load_sem = refs[-4:]
    width = line_ref.shape[2]
    step = pl.program_id(0)
    steps = pl.num_programs(0)
    mine = lax.axis_index("plane")
    core = lax.rem(lax.axis_index("tile"), 2)
    near = mine + 1 - 2 * lax.rem(mine, 2)
    far = mine + 2 - 4 * lax.rem(mine // 2, 2)
    partner = near * (1 - core) + far * core
    barrier = pltpu.get_barrier_semaphore()

    def fetch(index, k, part):
        slot = lax.rem(index, 2)
        source = pl.ds(pl.multiple_of(index * LANES + part * 32, 32), 32)
        lines = pl.ds(pl.multiple_of(part * 32, 32), 32)
        return pltpu.make_async_copy(
            grids[k].at[:, :, source, :],
            held_ref.at[slot, k, :, :, lines, :],
            load_sem.at[slot, k, part],
        )

    parts = LANES // 32

    @pl.when(step == 0)
    def _():
        for k in range(held):
            for part in range(parts):
                fetch(step, k, part).start()

    @pl.when((step > 0) & (step < steps - 1))
    def _():
        for k in range(held):
            for part in range(parts):
                fetch(step + 1, k, part).start()

    @pl.when(step == 0)
    def _():
        pl.semaphore_signal(
            barrier, inc=1, device_id={"plane": partner}, device_id_type=MESH
        )
        lane = lax.broadcasted_iota(jnp.int32, (DIGITS, width), 1)
        digit = lax.broadcasted_iota(jnp.int32, (DIGITS, width), 0)
        index = place(lane, partner, mine, own) * DIGITS + digit
        taps = [taps_ref[j] for j in range(taps_ref.shape[0])]
        angle, size = response(taps, index)
        line_ref[0] = 1.0 - squared(index)
        line_ref[1] = angle
        line_ref[2] = size * scale

        @pl.loop(0, WINDOW // 16)
        def _(i):
            at = pl.multiple_of(i * 16, 16)
            lane = lax.broadcasted_iota(jnp.int32, (16, width), 1)
            inner = lax.broadcasted_iota(jnp.int32, (16, width), 0) + at
            product = inner * place(lane, partner, mine, own)
            cos_d, sin_d = turn(product.astype(jnp.float32) * (1.0 / WINDOW))
            cos_s, sin_s = turn(inner.astype(jnp.float32) * (1.0 / G))
            upper, under = pl.ds(at, 16), pl.ds(WINDOW + at, 16)
            for b in range(DIGITS):
                real = cos_d.astype(jnp.bfloat16)
                weight_ref[b, 0, upper, :] = real
                weight_ref[b, 1, upper, :] = sin_d.astype(jnp.bfloat16)
                weight_ref[b, 0, under, :] = (-sin_d).astype(jnp.bfloat16)
                weight_ref[b, 1, under, :] = real
                cos_d, sin_d = cos_d * cos_s - sin_d * sin_s, cos_d * sin_s + sin_d * cos_s

        pl.semaphore_wait(barrier, 1)

    index = lax.axis_index("tile") * columns + step * LANES
    index = index + lax.broadcasted_iota(jnp.int32, (8, LANES), 1)
    taps = [
        jnp.full((8, LANES), taps_ref[j], jnp.float32).astype(jnp.bfloat16).astype(jnp.float32)
        for j in range(taps_ref.shape[0])
    ]
    angle, size = response(taps, index)
    for n, value in enumerate((squared(index), angle, size)):
        side_ref[n] = jnp.broadcast_to(value[0:1], (LANES, LANES)).T

    for k in range(held):
        grid_ref = held_ref.at[lax.rem(step, 2), k]

        @pl.loop(0, parts)
        def _(group):
            fetch(step, k, group).wait()
            for index in range(2):
                at = pl.multiple_of(group * 32 + index * 16, 16)
                part = pl.ds(at, 16)
                for half in range(WINDOW // LANES):
                    lanes = slice(half * LANES, (half + 1) * LANES)
                    for b0 in range(4):
                        heads = []
                        for w0 in range(4):
                            total = None
                            for w1 in range(4):
                                w = 4 * w1 + w0
                                value = quarter(
                                    (grid_ref[w, 0, part, lanes], grid_ref[w, 1, part, lanes]), w1 * b0
                                )
                                total = value if total is None else plus(total, value)
                            total = rotate(total, w0 * b0)
                            heads.append(total)
                        even, odd = plus(heads[0], heads[2]), minus(heads[0], heads[2])
                        even2, odd2 = plus(heads[1], heads[3]), minus(heads[1], heads[3])
                        odd2 = quarter(odd2, 1)
                        results = (plus(even, even2), plus(odd, odd2), minus(even, even2), minus(odd, odd2))
                        for b1, (re, im) in enumerate(results):
                            b = b0 + 4 * b1
                            rows = pl.ds(k * LANES + at, 16)
                            mixed_ref[b, half, rows, :] = re.astype(jnp.bfloat16)
                            mixed_ref[b, 2 + half, rows, :] = im.astype(jnp.bfloat16)

    @pl.when((step == 0) & (steps > 1))
    def _():
        for k in range(held):
            for part in range(parts):
                fetch(step + 1, k, part).start()

    def spectrum(b, full_ref):
        mixed = jnp.concatenate([mixed_ref[b, part] for part in range(4)], axis=1)
        weight = jnp.concatenate([weight_ref[b, part] for part in range(2)], axis=1)
        full_ref[...] = jnp.dot(mixed, weight, preferred_element_type=jnp.float32)

    def screen(b, full_ref):
        square = line_ref[0, pl.ds(b, 1), :] - side_ref[0]
        angle = line_ref[1, pl.ds(b, 1), :] + side_ref[1]
        drop = square * lax.rsqrt(square) - 1.0
        picture = None
        for k in range(held):
            rows = slice(k * LANES, (k + 1) * LANES)
            cos_s, sin_s = turn(w_ref[k : k + 1, :] * drop + angle, SHORT_COS, SHORT_SIN)
            value = cos_s * full_ref[rows, :width] - sin_s * full_ref[rows, width:]
            picture = value if picture is None else picture + value
        picture = (picture * (line_ref[2, pl.ds(b, 1), :] * side_ref[2])).T
        send_ref[step, b] = picture[:own]
        own_ref[0, b] = picture[own : 2 * own]

    def copy(index, piece):
        lines = pl.ds(piece * PIECE, PIECE)
        return pltpu.make_async_remote_copy(
            src_ref=send_ref.at[index, lines],
            dst_ref=got_ref.at[index, lines],
            send_sem=send_sem.at[index, piece],
            recv_sem=got_sem.at[index, piece],
            device_id={"plane": partner},
            device_id_type=MESH,
        )

    spectrum(0, even_ref)

    @pl.loop(0, DIGITS // PIECE)
    def _(piece):
        for pair in range(PIECE // 2):
            b = piece * PIECE + pair * 2
            spectrum(b + 1, odd_ref)
            screen(b, even_ref)
            spectrum(lax.rem(b + 2, DIGITS), even_ref)
            screen(b + 1, odd_ref)
        copy(step, piece).start()

    @pl.when(step == steps - 1)
    def _():
        for index in range(send_ref.shape[0]):
            for piece in range(DIGITS // PIECE):
                copy(index, piece).wait()


def sum_kernel(own_ref, got_ref, image_ref, left_ref, right_ref, out_ref, load_sem, done_sem):
    steps = left_ref.shape[0]

    def load(index):
        return (
            pltpu.make_async_copy(own_ref.at[index], left_ref.at[index], load_sem.at[0, index]),
            pltpu.make_async_copy(got_ref.at[index], right_ref.at[index], load_sem.at[1, index]),
        )

    def store(index):
        lanes = pl.ds(index * LANES, LANES)
        return pltpu.make_async_copy(
            out_ref.at[index], image_ref.at[:, :, lanes], done_sem.at[index]
        )

    for index in range(steps):
        for copy in load(index):
            copy.start()
    for index in range(steps):
        for copy in load(index):
            copy.wait()
        for b in range(DIGITS):
            out_ref[index, :, b, :] = left_ref[index, b] + right_ref[index, b]
        store(index).start()
    for index in range(steps):
        store(index).wait()


def local(visibility, target, offset, taps, w_plane):
    tiles = lax.axis_size("tile")
    planes = lax.axis_size("plane")
    devices = tiles * planes
    vis_dev = visibility.shape[1]
    capacity = 2 * vis_dev // devices
    slots = devices * capacity
    blocks = slots // LANES
    band = G // tiles
    columns = G // tiles
    windows = band // WINDOW
    own = G // planes // DIGITS
    width = max(LANES, 2 * own)
    held = planes // 2
    assert windows in (1, 2)
    vmem = pl.BlockSpec(memory_space=pltpu.VMEM)
    smem = pl.BlockSpec(memory_space=pltpu.SMEM)

    numbers = range(planes)
    jumps = [[d for d in numbers if not d & bit] for bit in (1, 2)]
    gathered, level = pl.pallas_call(
        functools.partial(front_kernel, windows, tiles, jumps),
        out_shape=[
            jax.ShapeDtypeStruct((tiles, 3 * blocks + 8, LANES), jnp.float32),
            jax.ShapeDtypeStruct((held, LANES), jnp.float32),
        ],
        in_specs=[pl.BlockSpec(memory_space=pl.ANY)] * 3 + [smem],
        out_specs=[vmem] * 2,
        scratch_shapes=[
            pltpu.VMEM((2, vis_dev), jnp.float32),
            pltpu.VMEM((vis_dev // LANES, LANES), jnp.int32),
            pltpu.VMEM((vis_dev // LANES, LANES), jnp.int32),
            pltpu.SemaphoreType.DMA((3,)),
            pltpu.VMEM((9 * devices, vis_dev), jnp.bfloat16),
            pltpu.VMEM((LANES, vis_dev), jnp.bfloat16),
            pltpu.VMEM((9 * blocks, devices * LANES), jnp.bfloat16),
            pltpu.VMEM((LANES, devices * LANES), jnp.bfloat16),
            pltpu.VMEM((devices, 4, LANES), jnp.float32),
            pltpu.VMEM((devices, 4, LANES), jnp.float32),
            pltpu.VMEM((tiles, 3 * blocks + 8, LANES), jnp.float32),
            pltpu.SemaphoreType.DMA((devices,)),
            pltpu.SemaphoreType.DMA((devices,)),
            pltpu.SemaphoreType.DMA((tiles,)),
            pltpu.SemaphoreType.DMA((tiles,)),
        ],
        compiler_params=pltpu.CompilerParams(collective_id=1, has_side_effects=True),
    )(
        visibility,
        target.reshape(-1, LANES),
        offset.reshape(-1, LANES),
        w_plane,
    )

    lists = [gathered]
    for k in range(1, held):
        moves = []
        for q in range(planes):
            for t in range(tiles):
                moves.append((q * tiles + t, (q ^ jumps[t % 2][k]) * tiles + t))
        lists.append(lax.ppermute(gathered, ("plane", "tile"), moves))

    def transform(slots_of):
        return pl.pallas_call(
            functools.partial(grid_kernel, windows, columns),
            out_shape=jax.ShapeDtypeStruct((DIGITS, 2 * columns, WINDOW), jnp.float32),
            in_specs=[pl.BlockSpec(memory_space=pl.ANY)],
            out_specs=pl.BlockSpec(memory_space=pl.ANY),
            scratch_shapes=[
                pltpu.VMEM((WIDE // LANES, 2 * columns + 16, LANES), jnp.bfloat16),
                pltpu.VMEM((WIDE // LANES, WINDOW + 16, LANES), jnp.bfloat16),
                pltpu.VMEM((2, BLOCK + 8, WIDE + LANES), jnp.float32),
                pltpu.VMEM((2, 8, WIDE), jnp.float32),
                pltpu.VMEM((2, 2 * columns, WINDOW), jnp.float32),
                pltpu.VMEM((tiles, 3 * blocks + 8, LANES), jnp.float32),
                pltpu.SemaphoreType.DMA((2,)),
                pltpu.SemaphoreType.DMA((tiles,)),
            ],
            cost_estimate=pl.CostEstimate(
                flops=2 * slots * tiles * columns * WINDOW, bytes_accessed=1 << 24, transcendentals=0
            ),
        )(slots_of).reshape(DIGITS, 2, columns, WINDOW)

    grids = [transform(v) for v in lists]

    steps = columns // LANES
    mine_part, other_part = pl.pallas_call(
        functools.partial(image_kernel, held, own, columns, 1.0 / math.sqrt(vis_dev * devices)),
        grid=(steps,),
        out_shape=[jax.ShapeDtypeStruct((steps, DIGITS, own, LANES), jnp.float32)] * 2,
        in_specs=[
            smem,
            vmem,
        ]
        + [pl.BlockSpec(memory_space=pl.ANY)] * held,
        out_specs=[
            pl.BlockSpec((1, DIGITS, own, LANES), lambda j: (j, 0, 0, 0)),
            pl.BlockSpec(memory_space=pl.ANY),
        ],
        scratch_shapes=[
            pltpu.VMEM((DIGITS, 4, held * LANES, LANES), jnp.bfloat16),
            pltpu.VMEM((held * LANES, 2 * width), jnp.float32),
            pltpu.VMEM((held * LANES, 2 * width), jnp.float32),
            pltpu.VMEM((steps, DIGITS, own, LANES), jnp.float32),
            pltpu.VMEM((DIGITS, 2, 2 * WINDOW, width), jnp.bfloat16),
            pltpu.VMEM((3, DIGITS, width), jnp.float32),
            pltpu.VMEM((3, LANES, LANES), jnp.float32),
            pltpu.VMEM((2, held, DIGITS, 2, LANES, WINDOW), jnp.float32),
            pltpu.SemaphoreType.DMA((steps, DIGITS // PIECE)),
            pltpu.SemaphoreType.DMA((steps, DIGITS // PIECE)),
            pltpu.SemaphoreType.DMA((2, held, LANES // 32)),
        ],
        compiler_params=pltpu.CompilerParams(
            collective_id=0,
            has_side_effects=True,
            vmem_limit_bytes=60 * 1024 * 1024,
            dimension_semantics=("arbitrary",),
        ),
    )(taps, level, *grids)
    anywhere = pl.BlockSpec(memory_space=pl.ANY)
    image = pl.pallas_call(
        sum_kernel,
        out_shape=jax.ShapeDtypeStruct((own, DIGITS, columns), jnp.float32),
        in_specs=[anywhere] * 2,
        out_specs=anywhere,
        scratch_shapes=[
            pltpu.VMEM((steps, DIGITS, own, LANES), jnp.float32),
            pltpu.VMEM((steps, DIGITS, own, LANES), jnp.float32),
            pltpu.VMEM((steps, own, DIGITS, LANES), jnp.float32),
            pltpu.SemaphoreType.DMA((2, steps)),
            pltpu.SemaphoreType.DMA((steps,)),
        ],
    )(mine_part, other_part)
    return image.reshape(own * DIGITS, columns)


def solution(mesh):
    return jax.shard_map(
        local,
        mesh=mesh,
        in_specs=(
            P(None, ("plane", "tile")),
            P(("plane", "tile"), None),
            P(("plane", "tile")),
            P(),
            P("plane"),
        ),
        out_specs=P("plane", "tile"),
        check_vma=False,
    )
```

```python
import functools
import math

import jax
import jax.numpy as jnp
import numpy as np
from jax import lax
from jax.experimental import pallas as pl
from jax.experimental.pallas import tpu as pltpu
from jax.sharding import PartitionSpec as P

G = 4096
LANES = 128
WINDOW = 256
DIGITS = G // WINDOW
BLOCK = 64
PIECE = 4
WIDE = 1024
HALF = 512
NARROW = 256
LARGE = WIDE + NARROW
MESH = pl.DeviceIdType.MESH


def fitted(function, terms):
    nodes = np.cos((np.arange(400) + 0.5) * np.pi / 400)
    square = 0.125 * (nodes + 1.0)
    table = np.polynomial.chebyshev.Chebyshev.fit(
        square, function(np.sqrt(square)), terms - 1, domain=[0.0, 0.25]
    )
    return [float(v) for v in table.convert(kind=np.polynomial.Polynomial).coef]


COS_COEF = fitted(lambda x: np.cos(2.0 * np.pi * x), 7)
SIN_COEF = fitted(lambda x: np.sin(2.0 * np.pi * x) / x, 6)


SHORT_COS = fitted(lambda x: np.cos(2.0 * np.pi * x), 6)
SHORT_SIN = fitted(lambda x: np.sin(2.0 * np.pi * x) / x, 5)


def horner(coefficients, x):
    total = coefficients[-1]
    for value in coefficients[-2::-1]:
        total = total * x + value
    return total


def turn(cycles, cos_terms=COS_COEF, sin_terms=SIN_COEF):
    part = cycles - jnp.round(cycles)
    square = part * part
    return horner(cos_terms, square), part * horner(sin_terms, square)


def pieces(value):
    high = value.astype(jnp.bfloat16).astype(jnp.float32)
    rest = value - high
    middle = rest.astype(jnp.bfloat16).astype(jnp.float32)
    return high, middle, rest - middle


def strict_upper(n):
    return jnp.where(
        lax.broadcasted_iota(jnp.int32, (n, n), 0) < lax.broadcasted_iota(jnp.int32, (n, n), 1),
        1.0,
        0.0,
    ).astype(jnp.bfloat16)


NT = (((1,), (1,)), ((), ()))


def flip(value, bits):
    bit = 1
    while bit <= bits:
        if bits & bit:
            value = value + bit - 2 * bit * lax.rem(value // bit, 2)
        bit *= 2
    return value


def front_kernel(
    windows, tiles, jumps, vis_in, target_in, offset_in, w_ref, out_ref, level_ref,
    vis_ref, target_ref, offset_ref, in_sem, lhs_ref, rhs_ref, left_ref, right_ref, send_ref, got_ref, ring_ref,
    send_sem, got_sem, pass_sem, ring_sem,
):
    devices = send_ref.shape[0]
    plane, tile = lax.axis_index("plane"), lax.axis_index("tile")
    mine = plane * tiles + tile
    barrier = pltpu.get_barrier_semaphore()
    inputs = [
        pltpu.make_async_copy(source, target, in_sem.at[n])
        for n, (source, target) in enumerate(
            ((vis_in, vis_ref), (target_in, target_ref), (offset_in, offset_ref))
        )
    ]
    for copy in inputs:
        copy.start()

    def seat(device):
        return {"plane": device // tiles, "tile": lax.rem(device, tiles)}

    @pl.loop(1, devices)
    def _(i):
        pl.semaphore_signal(
            barrier, inc=1, device_id=seat(lax.rem(mine + i, devices)), device_id_type=MESH
        )

    for copy in inputs:
        copy.wait()
    blocks = target_ref.shape[0]
    upper = strict_upper(LANES)
    line = lax.broadcasted_iota(jnp.int32, (devices, LANES), 0)
    slot = lax.broadcasted_iota(jnp.int32, (LANES, LANES), 0).astype(jnp.float32)
    carry = jnp.zeros((devices, 1), jnp.float32)
    for k in range(blocks):
        part = slice(k * LANES, (k + 1) * LANES)
        hit = line == target_ref[k : k + 1, :]
        hot = jnp.where(hit, 1.0, 0.0)
        before = jnp.dot(hot.astype(jnp.bfloat16), upper, preferred_element_type=jnp.float32)
        rank = jnp.sum(hot * (before + carry), axis=0, keepdims=True)
        carry = carry + jnp.sum(hot, axis=1, keepdims=True)
        rhs_ref[:, part] = jnp.where(slot == rank, 1.0, 0.0).astype(jnp.bfloat16)
        rows = (
            vis_ref[0:1, part],
            vis_ref[1:2, part],
            offset_ref[k : k + 1, :].astype(jnp.float32) + 1.0,
        )
        for p, row in enumerate(rows):
            for n, value in enumerate(pieces(row)):
                at = (p * 3 + n) * devices
                lhs_ref[at : at + devices, part] = jnp.where(hit, value, 0.0).astype(jnp.bfloat16)
    total = lax.dot_general(lhs_ref[...], rhs_ref[...], NT, preferred_element_type=jnp.float32)
    for p in range(3):
        at = p * 3 * devices
        send_ref[:, p, :] = (
            total[at : at + devices]
            + total[at + devices : at + 2 * devices]
            + total[at + 2 * devices : at + 3 * devices]
        )
    send_ref[:, 3, :] = jnp.full((devices, LANES), w_ref[0], jnp.float32)
    got_ref[mine] = send_ref[mine]
    pl.semaphore_wait(barrier, devices - 1)

    def post(source, target):
        return pltpu.make_async_remote_copy(
            src_ref=send_ref.at[target],
            dst_ref=got_ref.at[source],
            send_sem=send_sem.at[target],
            recv_sem=got_sem.at[source],
            device_id=seat(target),
            device_id_type=MESH,
        )

    @pl.loop(1, devices)
    def _(i):
        post(mine, lax.rem(mine + i, devices)).start()

    @pl.loop(1, devices)
    def _(i):
        post(lax.rem(mine + devices - i, devices), mine).wait_recv()

    for k in range(level_ref.shape[0]):
        near, far = flip(plane, jumps[0][k]), flip(plane, jumps[1][k])
        core = lax.rem(tile, 2)
        origin = (near * (1 - core) + far * core) * tiles + tile
        level_ref[k : k + 1, :] = got_ref[origin, 3:4, :]

    rows = left_ref.shape[0] // 9
    encoded = got_ref[:, 2, :]
    row = jnp.floor((encoded - 1.0) * (1.0 / G))
    lower = jnp.where(
        lax.broadcasted_iota(jnp.int32, (devices, devices), 0)
        > lax.broadcasted_iota(jnp.int32, (devices, devices), 1),
        1.0,
        0.0,
    ).astype(jnp.bfloat16)
    position = jnp.full(row.shape, -1.0, jnp.float32)
    for w in range(windows):
        member = jnp.where((row >= w * WINDOW) & (row < (w + 1) * WINDOW), 1.0, 0.0)
        flags = member.astype(jnp.bfloat16)
        inside = jnp.dot(flags, upper, preferred_element_type=jnp.float32)
        ahead = jnp.sum(
            jnp.dot(lower, flags, preferred_element_type=jnp.float32), axis=1, keepdims=True
        )
        place = inside + ahead
        number = jnp.sum(jnp.sum(member, axis=1, keepdims=True), axis=0, keepdims=True)
        ring_ref[tile, 3 * rows + w : 3 * rows + w + 1] = jnp.broadcast_to(number, (1, LANES))
        if w == 1:
            place = rows * LANES - 1 - place
        position = jnp.where(member > 0.0, place, position)
    high = jnp.floor(position * (1.0 / LANES))
    low = position - high * LANES
    line = lax.broadcasted_iota(jnp.int32, (rows, LANES), 0).astype(jnp.float32)
    parts = [pieces(got_ref[:, 0, :]), pieces(got_ref[:, 1, :]), pieces(encoded)]
    for k in range(devices):
        part = slice(k * LANES, (k + 1) * LANES)
        hit = line == high[k : k + 1, :]
        right_ref[:, part] = jnp.where(slot == low[k : k + 1, :], 1.0, 0.0).astype(jnp.bfloat16)
        for p in range(3):
            for n in range(3):
                at = (p * 3 + n) * rows
                left_ref[at : at + rows, part] = jnp.where(
                    hit, parts[p][n][k : k + 1, :], 0.0
                ).astype(jnp.bfloat16)
    total = lax.dot_general(left_ref[...], right_ref[...], NT, preferred_element_type=jnp.float32)
    for p in range(3):
        at = p * 3 * rows
        ring_ref[tile, p * rows : (p + 1) * rows] = (
            total[at : at + rows]
            + total[at + rows : at + 2 * rows]
            + total[at + 2 * rows : at + 3 * rows]
        )

    ring_ref[tile, 3 * rows + windows :] = jnp.zeros((8 - windows, LANES), jnp.float32)
    sister = tile + 1 - 2 * lax.rem(tile, 2)

    def hand(block, target, index):
        return pltpu.make_async_remote_copy(
            src_ref=ring_ref.at[block],
            dst_ref=ring_ref.at[block],
            send_sem=pass_sem.at[index],
            recv_sem=ring_sem.at[block],
            device_id={"tile": target},
            device_id_type=MESH,
        )

    steps = tiles // 2
    hand(tile, sister, 0).start()
    for i in range(1, steps):
        hand(tile, lax.rem(tile + 2 * i, tiles), i).start()
    for i in range(1, steps):
        block = lax.rem(tile + tiles - 2 * i, tiles)
        hand(block, sister, 0).wait_recv()
        hand(block, sister, steps + i).start()
    hand(sister, sister, 0).wait_recv()
    for i in range(1, steps):
        hand(lax.rem(sister + tiles - 2 * i, tiles), sister, 0).wait_recv()
    out_ref[...] = ring_ref[...]
    hand(tile, sister, 0).wait_send()
    for i in range(1, steps):
        hand(tile, lax.rem(tile + 2 * i, tiles), i).wait_send()
        hand(tile, sister, steps + i).wait_send()

    @pl.loop(1, devices)
    def _(i):
        post(mine, lax.rem(mine + i, devices)).wait_send()


def spread(re, im, leads_cos, leads_sin):
    half = len(leads_cos)
    low, high = [], []
    for cos_l, sin_l in zip(leads_cos, leads_sin):
        a, b = re * cos_l, im * sin_l
        c, d = im * cos_l, re * sin_l
        high.append((a - b, c + d))
        low.append((a + b, c - d))
    assert len(low) == half
    return low[::-1] + high


def grid_kernel(
    windows, columns, list_ref, grid_ref, table_ref, hot_ref, near_ref, lead_ref, sum_ref, vis_ref,
    done_sem, load_sem,
):
    tiles = vis_ref.shape[0]

    def load(tile):
        return pltpu.make_async_copy(list_ref.at[tile], vis_ref.at[tile], load_sem.at[tile])

    @pl.loop(0, tiles)
    def _(tile):
        load(tile).start()

    blocks = (vis_ref.shape[1] - 8) // 3
    tops = columns // BLOCK
    base = lax.axis_index("tile") * columns + (tops - 1) * (BLOCK // 2) + 28
    eight = lax.broadcasted_iota(jnp.int32, (8, LANES), 0)
    start_at = (eight + base).astype(jnp.float32)
    lead_at = jnp.where(eight < 4, 4 + 8 * eight, 32 + 64 * (eight - 4)).astype(jnp.float32)
    lane = lax.broadcasted_iota(jnp.int32, (WINDOW, LANES), 0).astype(jnp.float32)

    def drain(item):
        slot = lax.rem(item, 2)
        return pltpu.make_async_copy(sum_ref.at[slot], grid_ref.at[item], done_sem.at[slot])

    @pl.loop(0, tiles * windows)
    def _(item):
        tile, window = item // windows, lax.rem(item, windows)

        @pl.when(window == 0)
        def _():
            load(tile).wait()

        @pl.when(item >= 2)
        def _():
            drain(item - 2).wait()

        fill(tile, window, blocks, tops, columns, start_at, lead_at, lane,
             vis_ref, sum_ref.at[lax.rem(item, 2)], table_ref, hot_ref, near_ref, lead_ref)
        drain(item).start()

    for item in range(max(0, tiles * windows - 2), tiles * windows):
        drain(item).wait()


def fill(
    tile, window, blocks, tops, columns, start_at, lead_at, lane,
    vis_ref, out_ref, table_ref, hot_ref, near_ref, lead_ref,
):
    number = vis_ref[tile, pl.ds(3 * blocks + window, 1), :][0, 0].astype(jnp.int32)
    lowest = (window * WINDOW).astype(jnp.float32)

    def build(group, row):
        part = slice(group * LANES, (group + 1) * LANES)
        vis_re = vis_ref[tile, pl.ds(row, 1), :]
        vis_im = vis_ref[tile, pl.ds(blocks + row, 1), :]
        encoded = vis_ref[tile, pl.ds(2 * blocks + row, 1), :] - 1.0
        line = jnp.floor(encoded * (1.0 / G))
        unit = (encoded - line * G) * (1.0 / G)
        hot_ref[group, :WINDOW] = jnp.where(lane == line - lowest, 1.0, 0.0).astype(jnp.bfloat16)
        start_cos, start_sin = turn(start_at * unit)
        lead_cos, lead_sin = turn(lead_at * unit)
        first_re = vis_re * start_cos - vis_im * start_sin
        first_im = vis_re * start_sin + vis_im * start_cos
        small = spread(
            first_re,
            first_im,
            [lead_cos[i : i + 1] for i in range(4)],
            [lead_sin[i : i + 1] for i in range(4)],
        )
        for i, (re, im) in enumerate(small):
            near_ref[0, 8 * i : 8 * i + 8, part] = re
            near_ref[1, 8 * i : 8 * i + 8, part] = im
        lead_ref[0, :, part] = lead_cos
        lead_ref[1, :, part] = lead_sin

    def widen(group):
        part = slice(group * LANES, (group + 1) * LANES)
        for i in range(tops // 2):
            cos_l = lead_ref[0, 4 + i : 5 + i, part]
            sin_l = lead_ref[1, 4 + i : 5 + i, part]
            for lines in range(0, BLOCK, 16):
                re = near_ref[0, lines : lines + 16, part]
                im = near_ref[1, lines : lines + 16, part]
                a, b = re * cos_l, im * sin_l
                c, d = im * cos_l, re * sin_l
                at = (i * BLOCK + lines) * 4
                for n, value in enumerate((a - b, a + b, c + d, c - d)):
                    table_ref[group, at + 16 * n : at + 16 * n + 16, :] = value.astype(
                        jnp.bfloat16
                    )

    def deliver(product, add):
        for i in range(tops // 2):
            for lines in range(0, BLOCK, 16):
                high = (tops // 2 + i) * BLOCK + lines
                low = (tops // 2 - 1 - i) * BLOCK + lines
                at = (i * BLOCK + lines) * 4
                for n, row in enumerate((high, low, columns + high, columns + low)):
                    value = product[at + 16 * n : at + 16 * n + 16]
                    if add:
                        value = value + out_ref[row : row + 16]
                    out_ref[row : row + 16] = value

    def chunk(row, width, add):
        for group in range(width // LANES):
            build(group, row + group)
        for group in range(width // LANES):
            widen(group)
        groups = range(width // LANES)
        left = jnp.concatenate([table_ref[group, : 2 * columns] for group in groups], axis=1)
        right = jnp.concatenate([hot_ref[group, :WINDOW] for group in groups], axis=1)
        deliver(lax.dot_general(left, right, NT, preferred_element_type=jnp.float32), add)

    def place(done, width):
        return jnp.where(window == 0, done, blocks - done - width // LANES)

    @pl.when(number <= NARROW)
    def _():
        chunk(place(0, NARROW), NARROW, False)

    @pl.when((number > NARROW) & (number <= HALF))
    def _():
        chunk(place(0, HALF), HALF, False)

    @pl.when((number > HALF) & (number <= HALF + NARROW))
    def _():
        chunk(place(0, HALF + NARROW), HALF + NARROW, False)

    rest = jnp.maximum(number - WIDE, 0)
    full = rest // WIDE
    tail = rest - full * WIDE
    short = (tail > 0) & (tail <= NARROW)
    full = full + jnp.where(tail > HALF, 1, 0)
    begin = jnp.where(short, LARGE // LANES, WIDE // LANES)

    @pl.when((number > HALF + NARROW) & jnp.logical_not(short))
    def _():
        chunk(place(0, WIDE), WIDE, False)

    @pl.when(short)
    def _():
        chunk(place(0, LARGE), LARGE, False)

    @pl.loop(0, full)
    def _(index):
        chunk(place(begin + index * (WIDE // LANES), WIDE), WIDE, True)

    @pl.when((tail > NARROW) & (tail <= HALF))
    def _():
        chunk(place(begin + full * (WIDE // LANES), HALF), HALF, True)


def place(lane, first, second, count):
    return lax.rem(jnp.where(lane < count, first * count + lane, second * count + lane - count), WINDOW)


def squared(index):
    cosine = jnp.where(index >= G // 2, index - G, index).astype(jnp.float32) * (0.5 / G)
    return cosine * cosine


def response(taps, index):
    real = imag = None
    for j, tap in enumerate(taps):
        cos_j, sin_j = turn((index * j).astype(jnp.float32) * (1.0 / G))
        real = tap * cos_j if real is None else real + tap * cos_j
        imag = tap * sin_j if imag is None else imag + tap * sin_j
    return jnp.arctan2(imag, real) * (0.5 / math.pi), jnp.sqrt(real * real + imag * imag)


def quarter(value, turns):
    re, im = value
    return ((re, im), (-im, re), (-re, -im), (im, -re))[turns % 4]


def rotate(value, sixteenths):
    value = quarter(value, sixteenths // 4)
    rest = sixteenths % 4
    if rest == 0:
        return value
    re, im = value
    if rest == 2:
        root = math.sqrt(0.5)
        return (re - im) * root, (re + im) * root
    c, s = math.cos(rest * math.pi / 8), math.sin(rest * math.pi / 8)
    return re * c - im * s, re * s + im * c


def plus(left, right):
    return left[0] + right[0], left[1] + right[1]


def minus(left, right):
    return left[0] - right[0], left[1] - right[1]


def image_kernel(held, own, columns, scale, taps_ref, w_ref, *refs):
    grids, own_ref, got_ref = refs[:held], refs[held], refs[held + 1]
    mixed_ref, even_ref, odd_ref, send_ref, weight_ref, line_ref, side_ref = refs[held + 2 : -4]
    held_ref, send_sem, got_sem, load_sem = refs[-4:]
    width = line_ref.shape[2]
    step = pl.program_id(0)
    steps = pl.num_programs(0)
    mine = lax.axis_index("plane")
    core = lax.rem(lax.axis_index("tile"), 2)
    near = mine + 1 - 2 * lax.rem(mine, 2)
    far = mine + 2 - 4 * lax.rem(mine // 2, 2)
    partner = near * (1 - core) + far * core
    barrier = pltpu.get_barrier_semaphore()

    def fetch(index, k, part):
        slot = lax.rem(index, 2)
        source = pl.ds(pl.multiple_of(index * LANES + part * 32, 32), 32)
        lines = pl.ds(pl.multiple_of(part * 32, 32), 32)
        return pltpu.make_async_copy(
            grids[k].at[:, :, source, :],
            held_ref.at[slot, k, :, :, lines, :],
            load_sem.at[slot, k, part],
        )

    parts = LANES // 32

    @pl.when(step == 0)
    def _():
        for k in range(held):
            for part in range(parts):
                fetch(step, k, part).start()

    @pl.when((step > 0) & (step < steps - 1))
    def _():
        for k in range(held):
            for part in range(parts):
                fetch(step + 1, k, part).start()

    @pl.when(step == 0)
    def _():
        pl.semaphore_signal(
            barrier, inc=1, device_id={"plane": partner}, device_id_type=MESH
        )
        lane = lax.broadcasted_iota(jnp.int32, (DIGITS, width), 1)
        digit = lax.broadcasted_iota(jnp.int32, (DIGITS, width), 0)
        index = place(lane, partner, mine, own) * DIGITS + digit
        taps = [taps_ref[j] for j in range(taps_ref.shape[0])]
        angle, size = response(taps, index)
        line_ref[0] = 1.0 - squared(index)
        line_ref[1] = angle
        line_ref[2] = size * scale

        @pl.loop(0, WINDOW // 16)
        def _(i):
            at = pl.multiple_of(i * 16, 16)
            lane = lax.broadcasted_iota(jnp.int32, (16, width), 1)
            inner = lax.broadcasted_iota(jnp.int32, (16, width), 0) + at
            product = inner * place(lane, partner, mine, own)
            cos_d, sin_d = turn(product.astype(jnp.float32) * (1.0 / WINDOW))
            cos_s, sin_s = turn(inner.astype(jnp.float32) * (1.0 / G))
            upper, under = pl.ds(at, 16), pl.ds(WINDOW + at, 16)
            for b in range(DIGITS):
                real = cos_d.astype(jnp.bfloat16)
                weight_ref[b, 0, upper, :] = real
                weight_ref[b, 1, upper, :] = sin_d.astype(jnp.bfloat16)
                weight_ref[b, 0, under, :] = (-sin_d).astype(jnp.bfloat16)
                weight_ref[b, 1, under, :] = real
                cos_d, sin_d = cos_d * cos_s - sin_d * sin_s, cos_d * sin_s + sin_d * cos_s

        pl.semaphore_wait(barrier, 1)

    index = lax.axis_index("tile") * columns + step * LANES
    index = index + lax.broadcasted_iota(jnp.int32, (8, LANES), 1)
    taps = [
        jnp.full((8, LANES), taps_ref[j], jnp.float32).astype(jnp.bfloat16).astype(jnp.float32)
        for j in range(taps_ref.shape[0])
    ]
    angle, size = response(taps, index)
    for n, value in enumerate((squared(index), angle, size)):
        side_ref[n] = jnp.broadcast_to(value[0:1], (LANES, LANES)).T

    for k in range(held):
        grid_ref = held_ref.at[lax.rem(step, 2), k]

        @pl.loop(0, parts)
        def _(group):
            fetch(step, k, group).wait()
            for index in range(2):
                at = pl.multiple_of(group * 32 + index * 16, 16)
                part = pl.ds(at, 16)
                for half in range(WINDOW // LANES):
                    lanes = slice(half * LANES, (half + 1) * LANES)
                    for b0 in range(4):
                        heads = []
                        for w0 in range(4):
                            total = None
                            for w1 in range(4):
                                w = 4 * w1 + w0
                                value = quarter(
                                    (grid_ref[w, 0, part, lanes], grid_ref[w, 1, part, lanes]), w1 * b0
                                )
                                total = value if total is None else plus(total, value)
                            total = rotate(total, w0 * b0)
                            heads.append(total)
                        even, odd = plus(heads[0], heads[2]), minus(heads[0], heads[2])
                        even2, odd2 = plus(heads[1], heads[3]), minus(heads[1], heads[3])
                        odd2 = quarter(odd2, 1)
                        results = (plus(even, even2), plus(odd, odd2), minus(even, even2), minus(odd, odd2))
                        for b1, (re, im) in enumerate(results):
                            b = b0 + 4 * b1
                            rows = pl.ds(k * LANES + at, 16)
                            mixed_ref[b, half, rows, :] = re.astype(jnp.bfloat16)
                            mixed_ref[b, 2 + half, rows, :] = im.astype(jnp.bfloat16)

    @pl.when((step == 0) & (steps > 1))
    def _():
        for k in range(held):
            for part in range(parts):
                fetch(step + 1, k, part).start()

    def spectrum(b, full_ref):
        mixed = jnp.concatenate([mixed_ref[b, part] for part in range(4)], axis=1)
        weight = jnp.concatenate([weight_ref[b, part] for part in range(2)], axis=1)
        full_ref[...] = jnp.dot(mixed, weight, preferred_element_type=jnp.float32)

    def screen(b, full_ref):
        square = line_ref[0, pl.ds(b, 1), :] - side_ref[0]
        angle = line_ref[1, pl.ds(b, 1), :] + side_ref[1]
        drop = square * lax.rsqrt(square) - 1.0
        picture = None
        for k in range(held):
            rows = slice(k * LANES, (k + 1) * LANES)
            cos_s, sin_s = turn(w_ref[k : k + 1, :] * drop + angle, SHORT_COS, SHORT_SIN)
            value = cos_s * full_ref[rows, :width] - sin_s * full_ref[rows, width:]
            picture = value if picture is None else picture + value
        picture = (picture * (line_ref[2, pl.ds(b, 1), :] * side_ref[2])).T
        send_ref[step, b] = picture[:own]
        own_ref[0, b] = picture[own : 2 * own]

    def copy(index, piece):
        lines = pl.ds(piece * PIECE, PIECE)
        return pltpu.make_async_remote_copy(
            src_ref=send_ref.at[index, lines],
            dst_ref=got_ref.at[index, lines],
            send_sem=send_sem.at[index, piece],
            recv_sem=got_sem.at[index, piece],
            device_id={"plane": partner},
            device_id_type=MESH,
        )

    spectrum(0, even_ref)

    @pl.loop(0, DIGITS // PIECE)
    def _(piece):
        for pair in range(PIECE // 2):
            b = piece * PIECE + pair * 2
            spectrum(b + 1, odd_ref)
            screen(b, even_ref)
            spectrum(lax.rem(b + 2, DIGITS), even_ref)
            screen(b + 1, odd_ref)
        copy(step, piece).start()

    @pl.when(step == steps - 1)
    def _():
        for index in range(send_ref.shape[0]):
            for piece in range(DIGITS // PIECE):
                copy(index, piece).wait()


def sum_kernel(own_ref, got_ref, image_ref, left_ref, right_ref, out_ref, load_sem, done_sem):
    steps = left_ref.shape[0]

    def load(index):
        return (
            pltpu.make_async_copy(own_ref.at[index], left_ref.at[index], load_sem.at[0, index]),
            pltpu.make_async_copy(got_ref.at[index], right_ref.at[index], load_sem.at[1, index]),
        )

    def store(index):
        lanes = pl.ds(index * LANES, LANES)
        return pltpu.make_async_copy(
            out_ref.at[index], image_ref.at[:, :, lanes], done_sem.at[index]
        )

    for index in range(steps):
        for copy in load(index):
            copy.start()
    for index in range(steps):
        for copy in load(index):
            copy.wait()
        for b in range(DIGITS):
            out_ref[index, :, b, :] = left_ref[index, b] + right_ref[index, b]
        store(index).start()
    for index in range(steps):
        store(index).wait()


def local(visibility, target, offset, taps, w_plane):
    tiles = lax.axis_size("tile")
    planes = lax.axis_size("plane")
    devices = tiles * planes
    vis_dev = visibility.shape[1]
    capacity = 2 * vis_dev // devices
    slots = devices * capacity
    blocks = slots // LANES
    band = G // tiles
    columns = G // tiles
    windows = band // WINDOW
    own = G // planes // DIGITS
    width = max(LANES, 2 * own)
    held = planes // 2
    assert windows in (1, 2)
    vmem = pl.BlockSpec(memory_space=pltpu.VMEM)
    smem = pl.BlockSpec(memory_space=pltpu.SMEM)

    numbers = range(planes)
    jumps = [[d for d in numbers if not d & bit] for bit in (1, 2)]
    gathered, level = pl.pallas_call(
        functools.partial(front_kernel, windows, tiles, jumps),
        out_shape=[
            jax.ShapeDtypeStruct((tiles, 3 * blocks + 8, LANES), jnp.float32),
            jax.ShapeDtypeStruct((held, LANES), jnp.float32),
        ],
        in_specs=[pl.BlockSpec(memory_space=pl.ANY)] * 3 + [smem],
        out_specs=[vmem] * 2,
        scratch_shapes=[
            pltpu.VMEM((2, vis_dev), jnp.float32),
            pltpu.VMEM((vis_dev // LANES, LANES), jnp.int32),
            pltpu.VMEM((vis_dev // LANES, LANES), jnp.int32),
            pltpu.SemaphoreType.DMA((3,)),
            pltpu.VMEM((9 * devices, vis_dev), jnp.bfloat16),
            pltpu.VMEM((LANES, vis_dev), jnp.bfloat16),
            pltpu.VMEM((9 * blocks, devices * LANES), jnp.bfloat16),
            pltpu.VMEM((LANES, devices * LANES), jnp.bfloat16),
            pltpu.VMEM((devices, 4, LANES), jnp.float32),
            pltpu.VMEM((devices, 4, LANES), jnp.float32),
            pltpu.VMEM((tiles, 3 * blocks + 8, LANES), jnp.float32),
            pltpu.SemaphoreType.DMA((devices,)),
            pltpu.SemaphoreType.DMA((devices,)),
            pltpu.SemaphoreType.DMA((tiles,)),
            pltpu.SemaphoreType.DMA((tiles,)),
        ],
        compiler_params=pltpu.CompilerParams(collective_id=1, has_side_effects=True),
    )(
        visibility,
        target.reshape(-1, LANES),
        offset.reshape(-1, LANES),
        w_plane,
    )

    lists = [gathered]
    for k in range(1, held):
        moves = []
        for q in range(planes):
            for t in range(tiles):
                moves.append((q * tiles + t, (q ^ jumps[t % 2][k]) * tiles + t))
        lists.append(lax.ppermute(gathered, ("plane", "tile"), moves))

    def transform(slots_of):
        return pl.pallas_call(
            functools.partial(grid_kernel, windows, columns),
            out_shape=jax.ShapeDtypeStruct((DIGITS, 2 * columns, WINDOW), jnp.float32),
            in_specs=[pl.BlockSpec(memory_space=pl.ANY)],
            out_specs=pl.BlockSpec(memory_space=pl.ANY),
            scratch_shapes=[
                pltpu.VMEM((LARGE // LANES, 2 * columns + 16, LANES), jnp.bfloat16),
                pltpu.VMEM((LARGE // LANES, WINDOW + 16, LANES), jnp.bfloat16),
                pltpu.VMEM((2, BLOCK + 8, LARGE + LANES), jnp.float32),
                pltpu.VMEM((2, 8, LARGE), jnp.float32),
                pltpu.VMEM((2, 2 * columns, WINDOW), jnp.float32),
                pltpu.VMEM((tiles, 3 * blocks + 8, LANES), jnp.float32),
                pltpu.SemaphoreType.DMA((2,)),
                pltpu.SemaphoreType.DMA((tiles,)),
            ],
            cost_estimate=pl.CostEstimate(
                flops=2 * slots * tiles * columns * WINDOW, bytes_accessed=1 << 24, transcendentals=0
            ),
        )(slots_of).reshape(DIGITS, 2, columns, WINDOW)

    grids = [transform(v) for v in lists]

    steps = columns // LANES
    mine_part, other_part = pl.pallas_call(
        functools.partial(image_kernel, held, own, columns, 1.0 / math.sqrt(vis_dev * devices)),
        grid=(steps,),
        out_shape=[jax.ShapeDtypeStruct((steps, DIGITS, own, LANES), jnp.float32)] * 2,
        in_specs=[
            smem,
            vmem,
        ]
        + [pl.BlockSpec(memory_space=pl.ANY)] * held,
        out_specs=[
            pl.BlockSpec((1, DIGITS, own, LANES), lambda j: (j, 0, 0, 0)),
            pl.BlockSpec(memory_space=pl.ANY),
        ],
        scratch_shapes=[
            pltpu.VMEM((DIGITS, 4, held * LANES, LANES), jnp.bfloat16),
            pltpu.VMEM((held * LANES, 2 * width), jnp.float32),
            pltpu.VMEM((held * LANES, 2 * width), jnp.float32),
            pltpu.VMEM((steps, DIGITS, own, LANES), jnp.float32),
            pltpu.VMEM((DIGITS, 2, 2 * WINDOW, width), jnp.bfloat16),
            pltpu.VMEM((3, DIGITS, width), jnp.float32),
            pltpu.VMEM((3, LANES, LANES), jnp.float32),
            pltpu.VMEM((2, held, DIGITS, 2, LANES, WINDOW), jnp.float32),
            pltpu.SemaphoreType.DMA((steps, DIGITS // PIECE)),
            pltpu.SemaphoreType.DMA((steps, DIGITS // PIECE)),
            pltpu.SemaphoreType.DMA((2, held, LANES // 32)),
        ],
        compiler_params=pltpu.CompilerParams(
            collective_id=0,
            has_side_effects=True,
            vmem_limit_bytes=60 * 1024 * 1024,
            dimension_semantics=("arbitrary",),
        ),
    )(taps, level, *grids)
    anywhere = pl.BlockSpec(memory_space=pl.ANY)
    image = pl.pallas_call(
        sum_kernel,
        out_shape=jax.ShapeDtypeStruct((own, DIGITS, columns), jnp.float32),
        in_specs=[anywhere] * 2,
        out_specs=anywhere,
        scratch_shapes=[
            pltpu.VMEM((steps, DIGITS, own, LANES), jnp.float32),
            pltpu.VMEM((steps, DIGITS, own, LANES), jnp.float32),
            pltpu.VMEM((steps, own, DIGITS, LANES), jnp.float32),
            pltpu.SemaphoreType.DMA((2, steps)),
            pltpu.SemaphoreType.DMA((steps,)),
        ],
    )(mine_part, other_part)
    return image.reshape(own * DIGITS, columns)


def solution(mesh):
    return jax.shard_map(
        local,
        mesh=mesh,
        in_specs=(
            P(None, ("plane", "tile")),
            P(("plane", "tile"), None),
            P(("plane", "tile")),
            P(),
            P("plane"),
        ),
        out_specs=P("plane", "tile"),
        check_vma=False,
    )
```
